32 devices in a mesh: mat: 4 (over x, core), frac: 8 (over z, y).
Axes of the slice: x: 2, y: 2, z: 4, core: 2. Of those that a mesh axis runs over, the one named last changes fastest.
Arguments:
- pressure_start: float32 [64, 512, 256], P('mat', 'frac'), may hold values from -6 to 6
- face_trans: float32 [3, 64, 512, 256], P(None, 'mat', 'frac'), may hold values from 0.2 to 2
- cell_coef: float32 [64, 512, 256], P('mat', 'frac'), may hold values from 0.05 to 0.5
- matrix_source: float32 [64, 512, 256], P('mat', 'frac'), may hold values from -6 to 6
- mortar_owner: int32 [16384, 1], P(('mat', 'frac')), may hold values from 0 to 31; in each aligned block of 512 rows (0 to 511, 512 to 1023, ...) at most 32 rows name the same one
- mortar_cell: int32 [16384], P(('mat', 'frac')), may hold values from 0 to 262143
- mortar_frac: int32 [16384], P(('mat', 'frac')), may hold values from 0 to 8191
- mortar_kappa: float32 [16384], P(('mat', 'frac')), may hold values from 0.5 to 2
- tiles: float32 [64, 4, 128, 128], P('frac'), may hold values from -0.25 to 0.25
- tile_cols: int32 [64, 4], P('frac'), may hold values from 0 to 63
- frac_diag: float32 [8192], P('frac'), may hold values from 4 to 8
- frac_source: float32 [8192], P('frac'), may hold values from -6 to 6
- fracture_start: float32 [8192], P('frac'), may hold values from -6 to 6
Outputs:
- pressure: float32 [64, 512, 256], P('mat', 'frac')
- fracture: float32 [8192], P('frac')
- flux: float32 [16384], P(('mat', 'frac'))
The draws below stay inside these ranges and needn't reach their ends.
Inputs may be any that keep to these rules, and one draw needn't show every extreme that they name: `mortar_owner`: among the 512 mortar cells of one device, at most 32 name the same owner, and in some devices some owner is named exactly 32 times.
All inputs are finite; a program needn't handle non-finite values.
Results may differ from the reference program's by a relative error of at most 0.00015.
Values sent between devices are 32-bit elements; how exact they have to be, the bound alone decides.
A program may use at most 128 MiB of HBM per device.

```python
import math
import jax
import jax.numpy as jnp
import numpy as np
from jax import lax

CX = 16
CY = 64
CZ = 256
MORT_DEV = 512
B = 128
TILES = 4
SWEEPS = 2
CG_ITERS = 3
OUTER = 2
NX = 64
NY = 512
CELLS = 262144
NB = 64
NF = 8192
M = 16384
CAP = 32
N_MAT = 4
N_FRAC = 8
DEVICES = 32


def set_ends(values, key, low, high):
    longest = values.shape.index(max(values.shape))
    spots = []
    for shift in (0, 1):
        where = [jax.random.randint(jax.random.fold_in(key, axis), (), 0, length) for axis, length in enumerate(values.shape)]
        where[longest] = (where[longest] + shift) % values.shape[longest]
        spots.append(tuple(where))
    return values.at[spots[0]].set(low).at[spots[1]].set(high)


def block_levels(own_key, shape, pieces, smallest, top_value):
    level = 1.0
    for dim, parts in pieces:
        draws = jax.random.uniform(jax.random.fold_in(jax.random.fold_in(own_key, 6), dim), (parts,), jnp.float32, smallest / len(pieces), top_value / len(pieces))
        level = level * jnp.repeat(jnp.exp(draws), shape[dim] // parts).reshape((-1,) + (1,) * (len(shape) - 1 - dim))
    return level


def shared_out(rng, own, number, rows, amount, top, most, slope):
    order = jax.random.permutation(rng, amount)
    crowded, ordinary = shares(amount, rows * top, most, slope, True), shares(amount, rows * top, most, slope, False)
    places = jnp.arange(amount)

    def named(lengths, turn):
        used = int((lengths > 0).sum())
        fixed = max(1, used // 4)
        moved = fixed + (places - fixed + turn * (used - fixed)) % max(1, amount - fixed)
        return jnp.zeros((amount,), jnp.int32).at[order[jnp.where(places < fixed, places, moved)]].set(jnp.asarray(lengths, jnp.int32))

    lengths = jnp.where(number % 4 == 0, named(crowded, number // 4), named(ordinary, number - number // 4 - 1))
    mixed = jax.random.permutation(jax.random.fold_in(own, 3), amount)
    donor, taker = mixed[0:amount // 2 * 2:2], mixed[1:amount // 2 * 2:2]
    slack = jnp.minimum(lengths[donor] - 1, most - lengths[taker]) // 2
    slack = jnp.where((donor == order[0]) | (taker == order[0]) | (lengths[taker] == 0), 0, jnp.maximum(slack, 0))
    moved = jax.random.randint(jax.random.fold_in(own, 4), (amount // 2,), 0, 1 << 20) % (slack + 1)
    lengths = lengths.at[donor].add(-moved).at[taker].add(moved)
    labels = jnp.searchsorted(jnp.cumsum(lengths), jnp.arange(rows * top), side="right").astype(jnp.int32)
    grid = labels.reshape(top, rows).T
    grid = grid[jax.random.permutation(jax.random.fold_in(own, 1), rows)]
    turn = jax.random.randint(jax.random.fold_in(own, 2), (rows, 1), 0, top)
    return jnp.take_along_axis(grid, (jnp.arange(top)[None, :] + turn) % top, axis=1)


def shares(count, total, limit, lean, full):
    portions = [(1 << 20) // math.isqrt(standing ** lean) + 1 for standing in range(1, count + 1)]
    largest = limit if full else min(limit, max(-(-total // count), total * portions[0] // sum(portions)))
    least = 1 if total - largest >= count - 1 else 0
    given, surplus = [largest] + [least] * (count - 1), total - largest - least * (count - 1)
    while surplus > 0:
        movable = [i for i in range(1, count) if given[i] < largest] or [i for i in range(1, count) if given[i] < limit]
        whole, left = sum([portions[i] for i in movable]), surplus
        for i in movable:
            addition = min(limit - given[i], max(1, left * portions[i] // whole), surplus)
            given[i] = given[i] + addition
            surplus = surplus - addition
    return np.array(given)


def normal_values(rng, extent, scale, limit, split=(), dtype=jnp.bfloat16):
    values = scale * jax.random.normal(rng, extent, jnp.float32)
    if split:
        values = values * block_levels(rng, extent, split, -0.22, 0.18)
    return jnp.clip(values, -limit, limit).astype(dtype)


def setup_inputs(seed: int = 0) -> dict:
    seeds = jax.random.split(jax.random.key(seed), 14)
    pressure_start = normal_values(seeds[0], (NX, NY, CZ), 1.0, 6.0, ((0, 4), (1, 8)), jnp.float32)
    face_trans = jnp.clip(jnp.exp(math.log(2.0) - 2.3025851 * jax.random.uniform(seeds[1], (3, NX, NY, CZ), jnp.float32) ** block_levels(seeds[1], (3, NX, NY, CZ), ((1, 4), (2, 8)), -0.2, 0.2)), 0.2, 2.0)
    cell_coef = jnp.clip(jnp.exp(math.log(0.5) - 2.3025851 * jax.random.uniform(seeds[2], (NX, NY, CZ), jnp.float32) ** block_levels(seeds[2], (NX, NY, CZ), ((0, 4), (1, 8)), -0.2, 0.2)), 0.05, 0.5)
    matrix_source = normal_values(seeds[3], (NX, NY, CZ), 1.0, 6.0, ((0, 4), (1, 8)), jnp.float32)
    mortar_owner_keys = jax.random.split(jax.random.fold_in(seeds[4], 1), M // MORT_DEV)
    mortar_owner_turns = jax.random.permutation(jax.random.fold_in(seeds[4], 3), M // MORT_DEV)
    mortar_owner = jax.vmap(lambda own, number: shared_out(jax.random.fold_in(seeds[4], 2), own, number, MORT_DEV, DEVICES, 1, CAP, 2))(mortar_owner_keys, mortar_owner_turns).reshape((M, 1))
    mortar_cell = set_ends(jax.random.randint(seeds[5], (M,), 0, CELLS), jax.random.fold_in(seeds[5], 1), 0, CELLS - 1).astype(jnp.int32)
    mortar_frac = set_ends(jax.random.randint(seeds[6], (M,), 0, NF), jax.random.fold_in(seeds[6], 1), 0, NF - 1).astype(jnp.int32)
    mortar_kappa = jnp.clip(jnp.exp(math.log(2.0) - 1.3862944 * jax.random.uniform(seeds[7], (M,), jnp.float32) ** block_levels(seeds[7], (M,), ((0, 32),), -0.2, 0.2)), 0.5, 2.0)
    tiles = normal_values(seeds[8], (NB, TILES, B, B), (TILES * B) ** -0.5, 0.25, ((0, 8),), jnp.float32)
    tile_cols = set_ends(jax.random.randint(seeds[9], (NB, TILES), 0, NB), jax.random.fold_in(seeds[9], 1), 0, NB - 1).astype(jnp.int32)
    frac_diag = jnp.clip(jnp.exp(math.log(8.0) - 0.6931472 * jax.random.uniform(seeds[10], (NF,), jnp.float32) ** block_levels(seeds[10], (NF,), ((0, 8),), -0.2, 0.2)), 4.0, 8.0)
    frac_source = normal_values(seeds[11], (NF,), 1.0, 6.0, ((0, 8),), jnp.float32)
    fracture_start = normal_values(seeds[12], (NF,), 1.0, 6.0, ((0, 8),), jnp.float32)
    return {"pressure_start": pressure_start, "face_trans": face_trans, "cell_coef": cell_coef, "matrix_source": matrix_source, "mortar_owner": mortar_owner, "mortar_cell": mortar_cell, "mortar_frac": mortar_frac, "mortar_kappa": mortar_kappa, "tiles": tiles, "tile_cols": tile_cols, "frac_diag": frac_diag, "frac_source": frac_source, "fracture_start": fracture_start}


relax_weight = 0.8


def shift_next(values, along):
    padding = [(0, 0)] * values.ndim
    padding[along] = (0, 1)
    return lax.slice_in_dim(jnp.pad(values, padding), 1, values.shape[along] + 1, axis=along)


def shift_prev(values, along):
    padding = [(0, 0)] * values.ndim
    padding[along] = (1, 0)
    return lax.slice_in_dim(jnp.pad(values, padding), 0, values.shape[along], axis=along)


def relax_grid(pressure, face_trans, cell_coef, matrix_source, source):
    tx_low = shift_prev(face_trans[0], 0)
    ty_low = shift_prev(face_trans[1], 1)
    tz_low = shift_prev(face_trans[2], 2)
    diagonal = cell_coef + face_trans[0] + tx_low + face_trans[1] + ty_low + face_trans[2] + tz_low
    applied = (diagonal * pressure - face_trans[0] * shift_next(pressure, 0) - tx_low * shift_prev(pressure, 0)
               - face_trans[1] * shift_next(pressure, 1) - ty_low * shift_prev(pressure, 1)
               - face_trans[2] * shift_next(pressure, 2) - tz_low * shift_prev(pressure, 2))
    return pressure + relax_weight * (matrix_source + source - applied) / diagonal


def fracture_apply(vector, tiles, tile_cols, frac_diag):
    size_b = tiles.shape[2]
    blocks = vector.reshape(-1, size_b)
    forward = jnp.einsum("rtij,rtj->ri", tiles, blocks[tile_cols], precision=lax.Precision.HIGHEST)
    backward = jnp.einsum("rtij,ri->rtj", tiles, blocks, precision=lax.Precision.HIGHEST)
    spread = jnp.zeros_like(blocks).at[tile_cols.reshape(-1)].add(backward.reshape(-1, size_b))
    return frac_diag * vector + 0.5 * (forward + spread).reshape(-1)


def reference(pressure_start, face_trans, cell_coef, matrix_source, mortar_owner, mortar_cell, mortar_frac, mortar_kappa, tiles, tile_cols, frac_diag, frac_source, fracture_start):
    cells = CX * CY * CZ
    pressure = pressure_start
    fracture = fracture_start
    place = mortar_owner[:, 0].astype(jnp.int32) * cells + mortar_cell.astype(jnp.int32)
    flux = jnp.zeros(mortar_kappa.shape, jnp.float32)
    for outer_no in range(OUTER):
        by_device = pressure.reshape(N_MAT, CX, N_FRAC, CY, CZ).transpose(0, 2, 1, 3, 4).reshape(-1)
        trace = by_device[place]
        flux = mortar_kappa * (trace - fracture[mortar_frac])
        load = jnp.zeros(fracture.shape, jnp.float32).at[mortar_frac].add(flux)
        target = frac_source + load
        residual = target - fracture_apply(fracture, tiles, tile_cols, frac_diag)
        direction = residual
        norm_now = jnp.sum(residual * residual)
        for step in range(CG_ITERS):
            image = fracture_apply(direction, tiles, tile_cols, frac_diag)
            alpha = norm_now / jnp.sum(direction * image)
            fracture = fracture + alpha * direction
            residual = residual - alpha * image
            norm_next = jnp.sum(residual * residual)
            direction = residual + (norm_next / norm_now) * direction
            norm_now = norm_next
        landed = jnp.zeros(by_device.shape, jnp.float32).at[place].add(flux)
        source = landed.reshape(N_MAT, N_FRAC, CX, CY, CZ).transpose(0, 2, 1, 3, 4).reshape(pressure.shape)
        for sweep_no in range(SWEEPS):
            pressure = relax_grid(pressure, face_trans, cell_coef, matrix_source, source)
    return pressure, fracture, flux
```

```python
import functools

import jax
import jax.numpy as jnp
from jax import lax
from jax.experimental import pallas as pl
from jax.experimental.pallas import tpu as pltpu
from jax.sharding import PartitionSpec as P

SWEEPS = 2
CG_ITERS = 3
OUTER = 2

MESH = pl.DeviceIdType.MESH
LANES = 128

relax_weight = 0.8


def split_parts(values, count):
    parts = []
    for _ in range(count - 1):
        part = values.astype(jnp.bfloat16)
        parts.append(part)
        values = values - part.astype(jnp.float32)
    parts.append(values.astype(jnp.bfloat16))
    return parts


def as_hot(mask):
    return mask.astype(jnp.float32).astype(jnp.bfloat16)


def dot_nn(a, b):
    return lax.dot_general(a, b, (((1,), (0,)), ((), ())), preferred_element_type=jnp.float32)


def dot_nt(a, b):
    return lax.dot_general(a, b, (((1,), (1,)), ((), ())), preferred_element_type=jnp.float32)


def total_of(values):
    return jnp.sum(values, axis=(0, 1), keepdims=True)


def coupled_kernel(n_frac, n_mat, *refs):
    (press_hbm, face_hbm, cell_hbm, msource_hbm, tiles_hbm, owner_ref, cells_ref, places_ref, kappa_in_ref, cols_ref,
     diag_ref, begin_ref, fsource_ref, out_hbm, own_ref, flux_out_ref, *scratch) = refs
    (grid_ref, tx_ref, ty_ref, tz_ref, inv_ref, cell_ref, msource_ref, base_ref, result_ref, tiles_ref, parts_ref,
     row_hot_ref, lane_hot_ref, side_ref, edge_ref, ty_edge_ref, ty_side_ref, mort_out_ref, mort_in_ref, vec_ref,
     dest_out_ref, dest_in_ref, mv_ref, vector_ref, rs_out_0, rs_in_0, ag_0, rs_out_1, rs_in_1, ag_1, part_out_ref, part_in_ref,
     back_out_ref, back_in_ref, local_sem, out_sem, mort_send, mort_recv, vec_send, vec_recv, mv_send, mv_recv,
     rs_send, rs_recv, ag_send, ag_recv, part_send, part_recv, back_send, back_recv, halo_send, halo_recv) = scratch
    rows, tiles_row, size_b = tiles_ref.shape[0], tiles_ref.shape[1], tiles_ref.shape[3]
    width_x, width_y, depth_z = inv_ref.shape
    grid_rows = width_x * width_y
    mortars = owner_ref.shape[1]
    devices = n_mat * n_frac
    capacity = 2 * mortars // devices
    per = LANES // capacity
    groups = devices // per
    slots = devices * capacity
    blocks = rows * n_frac
    tiles_all = rows * tiles_row
    lines_mv = tiles_all + rows
    share = blocks // devices
    sweeps = OUTER * SWEEPS
    f32, i32 = jnp.float32, jnp.int32
    me = lax.axis_index("frac")
    me_mat = lax.axis_index("mat")
    me_dev = me_mat * n_frac + me
    everyone = [(c, k) for c in range(n_mat) for k in range(n_frac) if c or k]

    barrier = pltpu.get_barrier_semaphore()
    for c, k in everyone:
        pl.semaphore_signal(
            barrier,
            inc=1,
            device_id={"mat": lax.rem(me_mat + c, n_mat), "frac": lax.rem(me + k, n_frac)},
            device_id_type=MESH,
        )

    def load(index, src, dst):
        copy = pltpu.make_async_copy(src, dst, local_sem.at[index])
        copy.start()
        return copy

    press_copy = load(0, press_hbm, grid_ref.at[0, pl.ds(1, width_x)])
    tx_copy = load(1, face_hbm.at[0], tx_ref.at[pl.ds(1, width_x)])
    ty_copy = load(2, face_hbm.at[1], ty_ref)
    tiles_copy = load(3, tiles_hbm, tiles_ref)
    tz_copy = load(4, face_hbm.at[2], tz_ref)
    cell_copy = load(5, cell_hbm, cell_ref)
    msource_copy = load(6, msource_hbm, msource_ref)

    sent = []

    def send(src, dst, send_sem, recv_sem, device):
        copy = pltpu.make_async_remote_copy(
            src_ref=src, dst_ref=dst, send_sem=send_sem, recv_sem=recv_sem, device_id=device, device_id_type=MESH
        )
        copy.start()
        return copy

    def take(ref, sem):
        pltpu.make_async_copy(ref, ref, sem).wait()

    def spread_to_all(source, landing, send_sem, recv_sem):
        for c, k in everyone:
            mat, frac = lax.rem(me_mat + c, n_mat), lax.rem(me + k, n_frac)
            send(source(mat * n_frac + frac), landing.at[me_dev], send_sem, recv_sem, {"mat": mat, "frac": frac})
        sent.append((landing.at[pl.ds(0, devices - 1)], send_sem))

    def spread_to_frac(source, landing, send_sem, recv_sem):
        for k in range(1, n_frac):
            send(source, landing.at[me], send_sem, recv_sem, {"frac": lax.rem(me + k, n_frac)})
        sent.append((landing.at[pl.ds(0, n_frac - 1)], send_sem))

    owner = owner_ref[...]
    named = lax.broadcasted_iota(i32, (devices, mortars), 0) == owner
    named_hot = as_hot(named)
    before = as_hot(lax.broadcasted_iota(i32, (mortars, mortars), 0) <= lax.broadcasted_iota(i32, (mortars, mortars), 1))
    counts = dot_nn(named_hot, before)
    rank = jnp.sum(jnp.where(named, counts, 0.0), axis=0, keepdims=True).astype(i32) - 1
    spot = lax.broadcasted_iota(i32, (LANES, mortars), 0)
    word = lax.rem(spot // capacity + (per - lax.rem(me_dev, per)), per)
    payload = jnp.where(word == 0, cells_ref[...].astype(f32), jnp.where(word == 1, places_ref[...].astype(f32), kappa_in_ref[...]))
    payload = jnp.where((word < 3) & (lax.rem(spot, capacity) == rank), payload, 0.0)
    outgoing = sum(dot_nt(named_hot, part) for part in split_parts(payload, 3))
    mort_out_ref[...] = outgoing.reshape(devices, 1, LANES)

    lane_line = lax.broadcasted_iota(i32, (1, LANES), 1)
    target_row = jnp.where((lane_line >= tiles_all) & (lane_line < lines_mv), me * rows + lane_line - tiles_all, -1)
    for r in range(rows):
        for t in range(tiles_row):
            target_row = jnp.where(lane_line == r * tiles_row + t, cols_ref[t, r], target_row)
    dest_out_ref[...] = target_row.astype(f32)

    pl.semaphore_wait(barrier, devices - 1)
    spread_to_all(lambda target: mort_out_ref.at[target], mort_in_ref, mort_send, mort_recv)
    mort_in_ref[me_dev] = mort_out_ref[me_dev]
    spread_to_frac(begin_ref, vec_ref.at[0], vec_send.at[0], vec_recv.at[0])
    spread_to_frac(dest_out_ref, dest_in_ref, vec_send.at[3], vec_recv.at[3])
    vec_ref[0, me] = begin_ref[...]
    dest_in_ref[me] = dest_out_ref[...]

    lanes = lax.broadcasted_iota(i32, (width_y, depth_z), 1)
    lines = lax.broadcasted_iota(i32, (width_y, depth_z), 0)
    next_mat, prev_mat = lax.rem(me_mat + 1, n_mat), lax.rem(me_mat + n_mat - 1, n_mat)
    next_frac, prev_frac = lax.rem(me + 1, n_frac), lax.rem(me + n_frac - 1, n_frac)
    halos = {}
    slow_sends = []

    def send_halo(sweep):
        sems = [(halo_send.at[sweep, d], halo_recv.at[sweep, d]) for d in range(4)]
        halos[sweep] = [
            send(grid_ref.at[sweep, width_x], grid_ref.at[sweep, 0], *sems[0], {"mat": next_mat}),
            send(grid_ref.at[sweep, 1], grid_ref.at[sweep, width_x + 1], *sems[1], {"mat": prev_mat}),
            send(edge_ref.at[sweep, 0], side_ref.at[sweep, 0], *sems[2], {"frac": next_frac}),
            send(edge_ref.at[sweep, 1], side_ref.at[sweep, 1], *sems[3], {"frac": prev_frac}),
        ]
        slow_sends.extend(halos[sweep])

    def wait_halo(sweep):
        for copy in halos[sweep]:
            copy.wait_recv()
        grid_ref[sweep, 0] = jnp.where(me_mat == 0, 0.0, grid_ref[sweep, 0])
        grid_ref[sweep, width_x + 1] = jnp.where(me_mat == n_mat - 1, 0.0, grid_ref[sweep, width_x + 1])
        side_ref[sweep, 0] = jnp.where(me == 0, 0.0, side_ref[sweep, 0])
        side_ref[sweep, 1] = jnp.where(me == n_frac - 1, 0.0, side_ref[sweep, 1])

    press_copy.wait()
    edge_ref[0, 0] = grid_ref[0, 1 : width_x + 1, width_y - 1, :]
    edge_ref[0, 1] = grid_ref[0, 1 : width_x + 1, 0, :]
    send_halo(0)
    tx_copy.wait()
    ty_copy.wait()
    ty_edge_ref[...] = ty_ref[:, width_y - 1, :]
    coef_copies = [
        send(tx_ref.at[width_x], tx_ref.at[0], halo_send.at[sweeps, 0], halo_recv.at[sweeps, 0], {"mat": next_mat}),
        send(ty_edge_ref, ty_side_ref, halo_send.at[sweeps, 2], halo_recv.at[sweeps, 2], {"frac": next_frac}),
    ]
    slow_sends.extend(coef_copies)
    spread_to_frac(fsource_ref, vec_ref.at[1], vec_send.at[1], vec_recv.at[1])
    spread_to_frac(diag_ref, vec_ref.at[2], vec_send.at[2], vec_recv.at[2])
    vec_ref[1, me] = fsource_ref[...]
    vec_ref[2, me] = diag_ref[...]

    def gathered(index):
        take(vec_ref.at[index, pl.ds(0, n_frac - 1)], vec_recv.at[index])
        return vec_ref[index].reshape(blocks, size_b)

    def set_parts(sweep):
        high, low = split_parts(grid_ref[sweep, 1 : width_x + 1].reshape(grid_rows, depth_z), 2)
        parts_ref[0] = high
        parts_ref[1] = low

    def set_inverse():
        tz_copy.wait()
        cell_copy.wait()
        for copy in coef_copies:
            copy.wait_recv()
        tx_ref[0] = jnp.where(me_mat == 0, 0.0, tx_ref[0])
        ty_side_ref[...] = jnp.where(me == 0, 0.0, ty_side_ref[...])

        def plane(x, carry):
            ty_here, tz_here = ty_ref[x], tz_ref[x]
            tz_in = jnp.where(lanes == depth_z - 1, 0.0, tz_here)
            ty_low = jnp.where(lines == 0, ty_side_ref[pl.ds(x, 1), :], pltpu.roll(ty_here, 1, 0))
            tz_low = pltpu.roll(tz_in, 1, 1)
            inv_ref[x] = relax_weight / (cell_ref[x] + tx_ref[x + 1] + tx_ref[x] + ty_here + ty_low + tz_here + tz_low)
            tz_ref[x] = tz_in
            return carry

        lax.fori_loop(0, width_x, plane, 0)

    def sweep_part(sweep, low, high):
        def plane(x, carry):
            here = grid_ref[sweep, x + 1]
            ty_here, tz_here = ty_ref[x], tz_ref[x]
            up = jnp.where(lines == width_y - 1, side_ref[sweep, 1, pl.ds(x, 1), :], pltpu.roll(here, width_y - 1, 0))
            down = jnp.where(
                lines == 0,
                ty_side_ref[pl.ds(x, 1), :] * side_ref[sweep, 0, pl.ds(x, 1), :],
                pltpu.roll(ty_here * here, 1, 0),
            )
            total = base_ref[x] + tx_ref[x + 1] * grid_ref[sweep, x + 2] + tx_ref[x] * grid_ref[sweep, x]
            total = total + ty_here * up + down
            total = total + tz_here * pltpu.roll(here, depth_z - 1, 1) + pltpu.roll(tz_here * here, 1, 1)
            value = (1.0 - relax_weight) * here + inv_ref[x] * total
            if sweep + 1 < sweeps:
                grid_ref[sweep + 1, x + 1] = value
                edge_ref[sweep + 1, 0, pl.ds(x, 1), :] = value[width_y - 1 :]
                edge_ref[sweep + 1, 1, pl.ds(x, 1), :] = value[:1]
            else:
                result_ref[x] = value
            return carry

        lax.fori_loop(low, high, plane, 0)

    set_parts(0)
    set_inverse()

    take(mort_in_ref.at[pl.ds(0, devices - 1)], mort_recv)
    arrived = mort_in_ref[...].reshape(devices, LANES)
    window = lax.broadcasted_iota(i32, (devices, LANES), 1) // capacity
    device = lax.broadcasted_iota(i32, (devices, LANES), 0)

    def slot_line(word_no):
        turned = pltpu.roll(arrived, LANES - word_no * capacity, 1) if word_no else arrived
        chosen = jnp.where(lax.rem(device, per) == window, turned, 0.0)
        return jnp.concatenate(
            [jnp.sum(chosen[g * per : (g + 1) * per], axis=0, keepdims=True) for g in range(groups)], axis=1
        )

    cell = slot_line(0).astype(i32)
    place = slot_line(1).astype(i32)
    kappa = slot_line(2)
    cell_row = cell // depth_z
    cell_lane = cell - cell_row * depth_z
    block_of = place // size_b
    lane_of = place - block_of * size_b
    lane_hot_ref[...] = as_hot(lax.broadcasted_iota(i32, (depth_z, slots), 0) == cell_lane)
    by_lane = as_hot(lax.broadcasted_iota(i32, (size_b, slots), 0) == lane_of)
    by_block = lax.broadcasted_iota(i32, (blocks, slots), 0) == block_of

    quarter = slots // 4
    grid_line = lax.broadcasted_iota(i32, (grid_rows, quarter), 0)

    def traces():
        found = []
        for q in range(4):
            hot = lane_hot_ref[:, q * quarter : (q + 1) * quarter]
            picked = dot_nn(parts_ref[0], hot) + dot_nn(parts_ref[1], hot)
            found.append(
                jnp.sum(jnp.where(grid_line == cell_row[:, q * quarter : (q + 1) * quarter], picked, 0.0), axis=0, keepdims=True)
            )
        return jnp.concatenate(found, axis=1)

    def at_slots(values):
        picked = sum(dot_nn(part, by_lane) for part in split_parts(values, 3))
        return jnp.sum(jnp.where(by_block, picked, 0.0), axis=0, keepdims=True)

    def landed(values):
        return sum(dot_nt(as_part, by_lane) for as_part in split_parts(jnp.where(by_block, values, 0.0), 3))

    shares = [(rs_out_0, rs_in_0, ag_0), (rs_out_1, rs_in_1, ag_1)]

    def scatter_share(stage, arrays):
        out, landing, _ = shares[stage]
        for n, array in enumerate(arrays):
            out[:, n] = array.reshape(devices, share, size_b)
        spread_to_all(lambda target: out.at[target], landing, rs_send.at[stage], rs_recv.at[stage])
        landing[me_dev] = out[me_dev]

    def gather_share(stage):
        _, landing, whole = shares[stage]
        take(landing.at[pl.ds(0, devices - 1)], rs_recv.at[stage])
        mine = landing[0]
        for d in range(1, devices):
            mine = mine + landing[d]
        whole[me_dev] = mine
        spread_to_all(lambda target: whole.at[me_dev], whole, ag_send.at[stage], ag_recv.at[stage])

    def whole_shares(stage):
        _, _, whole = shares[stage]
        take(whole.at[pl.ds(0, devices - 1)], ag_recv.at[stage])
        return [whole[:, n].reshape(blocks, size_b) for n in range(whole.shape[1])]

    def products(phase, with_back):
        def row(r, carry):
            across = vector_ref[phase, pl.ds(me * rows + r, 1), :]
            down = jnp.broadcast_to(across, (size_b, size_b)).T
            total = jnp.zeros((size_b, size_b), f32)
            for t in range(tiles_row):
                tile = tiles_ref[r, t]
                total = total + tile * vector_ref[phase, pl.ds(cols_ref[t, r], 1), :]
                if with_back:
                    mv_ref[phase, me, pl.ds(r * tiles_row + t, 1), :] = jnp.sum(tile * down, axis=0, keepdims=True)
            mv_ref[phase, me, pl.ds(tiles_all + r, 1), :] = jnp.sum(total.T, axis=0, keepdims=True)
            return carry

        lax.fori_loop(0, rows, row, 0)

    def start_matvec(phase, vector):
        vector_ref[phase] = vector
        products(phase, True)
        spread_to_frac(mv_ref.at[phase, me], mv_ref.at[phase], mv_send.at[phase], mv_recv.at[phase])

    def finish_matvec(phase, vector):
        take(mv_ref.at[phase, pl.ds(0, n_frac - 1)], mv_recv.at[phase])
        forward = mv_ref[phase, :, tiles_all:].reshape(blocks, size_b)
        product = total_of(vector * (diag * vector + forward))
        arrived = mv_ref[phase].reshape(n_frac * lines_mv, size_b)
        both = sum(dot_nn(targets, part) for part in split_parts(arrived, 3))
        return product, diag * vector + 0.5 * both

    def set_row_hot():
        line = lax.broadcasted_iota(i32, (grid_rows, quarter), 0)
        for q in range(4):
            cut = slice(q * quarter, (q + 1) * quarter)
            row_hot_ref[:, cut] = as_hot(line == cell_row[:, cut])

    part_x = width_x // 4

    def set_sources(flux):
        wide = lane_hot_ref[...]
        weights = [wide * part for part in split_parts(flux, 2)]
        for q in range(4):
            low = q * part_x
            hot = row_hot_ref[low * width_y : (low + part_x) * width_y, :]
            total = sum(dot_nt(hot, weight) for weight in weights)
            base_ref[low : low + part_x] = msource_ref[low : low + part_x] + total.reshape(part_x, width_y, depth_z)

    begin = gathered(0)
    trace = traces()
    flux = kappa * (trace - at_slots(begin))
    scatter_share(0, [landed(flux)])

    tiles_copy.wait()
    start_matvec(0, begin)
    set_row_hot()
    msource_copy.wait()
    set_sources(flux)
    take(dest_in_ref.at[pl.ds(0, n_frac - 1)], vec_recv.at[3])
    block_line = lax.broadcasted_iota(i32, (blocks, LANES), 0)
    targets = jnp.concatenate(
        [as_hot(block_line == dest_in_ref[d].astype(i32))[:, :lines_mv] for d in range(n_frac)], axis=1
    )
    fsource = gathered(1)
    diag = gathered(2)
    gather_share(0)

    wait_halo(0)
    sweep_part(0, 0, width_x)
    send_halo(1)
    _, image = finish_matvec(0, begin)
    (loaded,) = whole_shares(0)
    residual = fsource + loaded - image
    fracture = begin

    def fill(number):
        if number == 0:
            wait_halo(1)
            sweep_part(1, 0, width_x)
            send_halo(2)
            set_parts(2)
            state["trace"] = traces()
            scatter_share(1, [landed(kappa * state["trace"]), landed(kappa)])
        elif number == 2:
            gather_share(1)
        elif number == 3:
            flux = kappa * (state["trace"] - at_slots(state["fracture"]))
            for g in range(groups):
                back_out_ref[g] = flux[:, g * LANES : (g + 1) * LANES]
            spread_to_all(lambda target: back_out_ref.at[target // per], back_in_ref, back_send, back_recv)
            back_in_ref[me_dev] = back_out_ref[me_dev // per]
            set_sources(flux)
            wait_halo(2)
            sweep_part(2, 0, width_x)
            send_halo(3)
        elif number == 4:
            wait_halo(3)
            for q in range(4):
                part = pl.ds(q * part_x, part_x)
                sweep_part(3, q * part_x, (q + 1) * part_x)
                copy = pltpu.make_async_copy(result_ref.at[part], out_hbm.at[part], out_sem.at[q])
                copy.start()
                results.append(copy)
        elif number == 5:
            take(back_in_ref.at[pl.ds(0, devices - 1)], back_recv)
            came = back_in_ref[...].reshape(devices, LANES)
            lines_back = sum(
                lax.dot_general(part, named_hot, (((0,), (0,)), ((), ())), preferred_element_type=f32)
                for part in split_parts(came, 3)
            )
            want = rank + capacity * lax.rem(me_dev, per)
            flux_out_ref[...] = jnp.sum(jnp.where(spot == want, lines_back, 0.0), axis=0, keepdims=True)

    state = {}
    results = []
    last = OUTER * CG_ITERS - 1
    for number in range(OUTER * CG_ITERS):
        step = number % CG_ITERS
        phase = number + 1
        if number == CG_ITERS:
            traced, weight = whole_shares(1)
            residual = residual + ((traced - weight * fracture) - loaded)
            state["fracture"] = fracture
        if number < last:
            start_matvec(phase, residual)
        else:
            vector_ref[phase] = residual
            products(phase, False)
            mine = pl.ds(pl.multiple_of(me * rows, rows), rows)
            part_out_ref[...] = jnp.sum(
                vector_ref[phase, mine, :] * mv_ref[phase, me, tiles_all:, :], axis=0, keepdims=True
            )
            spread_to_frac(part_out_ref, part_in_ref, part_send, part_recv)
            part_in_ref[me] = part_out_ref[...]
        norm_next = total_of(residual * residual)
        fill(number)
        if number < last:
            product, image = finish_matvec(phase, residual)
        else:
            take(part_in_ref.at[pl.ds(0, n_frac - 1)], part_recv)
            product = total_of(diag * residual * residual)
            lines_all = part_in_ref[0]
            for d in range(1, n_frac):
                lines_all = lines_all + part_in_ref[d]
            product = product + total_of(lines_all)
        if step == 0:
            alpha = norm_next / product
            direction = residual
            along = image
        else:
            ratio = norm_next / norm_now
            alpha = norm_next / (product - ratio * norm_next / alpha)
            direction = residual + ratio * direction
            if number < last:
                along = image + ratio * along
        norm_now = norm_next
        fracture = fracture + alpha * direction
        if number < last:
            residual = residual - alpha * along

    vector_ref[0] = fracture
    own_ref[...] = vector_ref[0, pl.ds(pl.multiple_of(me * rows, rows), rows), :]
    for ref, sem in sent:
        take(ref, sem)
    for copy in slow_sends:
        copy.wait_send()
    for copy in results:
        copy.wait()


def coupled(pressure, face, cell_coef, matrix_source, tiles, owner, cells, places, kappa, tile_cols, diag, begin, fsource):
    n_frac, n_mat = lax.axis_size("frac"), lax.axis_size("mat")
    devices = n_frac * n_mat
    rows, tiles_row, size_b = tiles.shape[0], tiles.shape[1], tiles.shape[3]
    blocks = rows * n_frac
    x, y, z = pressure.shape
    mortars = owner.shape[1]
    capacity = 2 * mortars // devices
    slots = devices * capacity
    groups = slots // LANES
    share = blocks // devices
    lines_mv = rows * tiles_row + rows
    f32, bf16 = jnp.float32, jnp.bfloat16
    vmem = pl.BlockSpec(memory_space=pltpu.VMEM)
    smem = pl.BlockSpec(memory_space=pltpu.SMEM)
    hbm = pl.BlockSpec(memory_space=pl.ANY)
    phases = OUTER * CG_ITERS + 1
    sweeps = OUTER * SWEEPS
    dma = pltpu.SemaphoreType.DMA
    return pl.pallas_call(
        functools.partial(coupled_kernel, n_frac, n_mat),
        out_shape=(
            jax.ShapeDtypeStruct((x, y, z), f32),
            jax.ShapeDtypeStruct((rows, size_b), f32),
            jax.ShapeDtypeStruct((1, mortars), f32),
        ),
        in_specs=[hbm] * 5 + [vmem] * 4 + [smem] + [vmem] * 3,
        out_specs=(hbm, vmem, vmem),
        scratch_shapes=[
            pltpu.VMEM((sweeps, x + 2, y, z), f32),
            pltpu.VMEM((x + 1, y, z), f32),
            pltpu.VMEM((x, y, z), f32),
            pltpu.VMEM((x, y, z), f32),
            pltpu.VMEM((x, y, z), f32),
            pltpu.VMEM((x, y, z), f32),
            pltpu.VMEM((x, y, z), f32),
            pltpu.VMEM((x, y, z), f32),
            pltpu.VMEM((x, y, z), f32),
            pltpu.VMEM((rows, tiles_row, size_b, size_b), f32),
            pltpu.VMEM((2, x * y, z), bf16),
            pltpu.VMEM((x * y, slots), bf16),
            pltpu.VMEM((z, slots), bf16),
            pltpu.VMEM((sweeps, 2, x, z), f32),
            pltpu.VMEM((sweeps, 2, x, z), f32),
            pltpu.VMEM((x, z), f32),
            pltpu.VMEM((x, z), f32),
            pltpu.VMEM((devices, 1, LANES), f32),
            pltpu.VMEM((devices, 1, LANES), f32),
            pltpu.VMEM((3, n_frac, rows, size_b), f32),
            pltpu.VMEM((1, LANES), f32),
            pltpu.VMEM((n_frac, 1, LANES), f32),
            pltpu.VMEM((phases, n_frac, lines_mv, size_b), f32),
            pltpu.VMEM((phases, blocks, size_b), f32),
            pltpu.VMEM((devices, 1, share, size_b), f32),
            pltpu.VMEM((devices, 1, share, size_b), f32),
            pltpu.VMEM((devices, 1, share, size_b), f32),
            pltpu.VMEM((devices, 2, share, size_b), f32),
            pltpu.VMEM((devices, 2, share, size_b), f32),
            pltpu.VMEM((devices, 2, share, size_b), f32),
            pltpu.VMEM((1, size_b), f32),
            pltpu.VMEM((n_frac, 1, size_b), f32),
            pltpu.VMEM((groups, 1, LANES), f32),
            pltpu.VMEM((devices, 1, LANES), f32),
            dma((7,)),
            dma((4,)),
            dma,
            dma,
            dma((4,)),
            dma((4,)),
            dma((phases,)),
            dma((phases,)),
            dma((2,)),
            dma((2,)),
            dma((2,)),
            dma((2,)),
            dma,
            dma,
            dma,
            dma,
            dma((sweeps + 1, 4)),
            dma((sweeps + 1, 4)),
        ],
        compiler_params=pltpu.CompilerParams(
            collective_id=0, has_side_effects=True, vmem_limit_bytes=60 * 1024 * 1024
        ),
        name="coupled",
    )(pressure, face, cell_coef, matrix_source, tiles, owner, cells, places, kappa, tile_cols, diag, begin, fsource)


def body(
    pressure_start,
    face_trans,
    cell_coef,
    matrix_source,
    mortar_owner,
    mortar_cell,
    mortar_frac,
    mortar_kappa,
    tiles,
    tile_cols,
    frac_diag,
    frac_source,
    fracture_start,
):
    size_b = tiles.shape[2]
    line = (1, -1)
    blocked = (-1, size_b)
    pressure, fracture, flux = coupled(
        pressure_start,
        face_trans,
        cell_coef,
        matrix_source,
        tiles,
        mortar_owner.reshape(line),
        mortar_cell.reshape(line),
        mortar_frac.reshape(line),
        mortar_kappa.reshape(line),
        tile_cols.T,
        frac_diag.reshape(blocked),
        fracture_start.reshape(blocked),
        frac_source.reshape(blocked),
    )
    return (pressure, fracture.reshape(-1), flux.reshape(-1))


def solution(mesh):
    in_specs = (
        P("mat", "frac", None),
        P(None, "mat", "frac", None),
        P("mat", "frac", None),
        P("mat", "frac", None),
        P(("mat", "frac"), None),
        P(("mat", "frac")),
        P(("mat", "frac")),
        P(("mat", "frac")),
        P("frac", None, None, None),
        P("frac", None),
        P("frac"),
        P("frac"),
        P("frac"),
    )
    out_specs = (P("mat", "frac", None), P("frac"), P(("mat", "frac")))
    return jax.shard_map(body, mesh=mesh, in_specs=in_specs, out_specs=out_specs, check_vma=False)
```

```python
import functools

import jax
import jax.numpy as jnp
from jax import lax
from jax.experimental import pallas as pl
from jax.experimental.pallas import tpu as pltpu
from jax.sharding import PartitionSpec as P

SWEEPS = 2
CG_ITERS = 3
OUTER = 2

MESH = pl.DeviceIdType.MESH
LANES = 128

relax_weight = 0.8


def split_parts(values, count):
    parts = []
    for _ in range(count - 1):
        part = values.astype(jnp.bfloat16)
        parts.append(part)
        values = values - part.astype(jnp.float32)
    parts.append(values.astype(jnp.bfloat16))
    return parts


def as_hot(mask):
    return mask.astype(jnp.float32).astype(jnp.bfloat16)


def dot_nn(a, b):
    return lax.dot_general(a, b, (((1,), (0,)), ((), ())), preferred_element_type=jnp.float32)


def dot_nt(a, b):
    return lax.dot_general(a, b, (((1,), (1,)), ((), ())), preferred_element_type=jnp.float32)


def total_of(values):
    return jnp.sum(values, axis=(0, 1), keepdims=True)


def coupled_kernel(n_frac, n_mat, *refs):
    (press_hbm, face_hbm, cell_hbm, msource_hbm, tiles_hbm, owner_ref, cells_ref, places_ref, kappa_in_ref, cols_ref,
     diag_ref, begin_ref, fsource_ref, out_ref, own_ref, flux_out_ref, *scratch) = refs
    (grid_ref, tx_ref, ty_ref, tz_ref, inv_ref, cell_ref, msource_ref, base_ref, tiles_ref, parts_ref,
     row_hot_ref, lane_hot_ref, side_ref, edge_ref, ty_edge_ref, ty_side_ref, mort_out_ref, mort_in_ref, vec_ref,
     dest_out_ref, dest_in_ref, mv_ref, vector_ref, rs_out_0, rs_in_0, ag_0, rs_out_1, rs_in_1, ag_1, part_out_ref, part_in_ref,
     back_out_ref, back_in_ref, local_sem, mort_send, mort_recv, vec_send, vec_recv, mv_send, mv_recv,
     rs_send, rs_recv, ag_send, ag_recv, part_send, part_recv, back_send, back_recv, halo_send, halo_recv) = scratch
    rows, tiles_row, size_b = tiles_ref.shape[0], tiles_ref.shape[1], tiles_ref.shape[3]
    width_x, width_y, depth_z = inv_ref.shape
    grid_rows = width_x * width_y
    mortars = owner_ref.shape[1]
    devices = n_mat * n_frac
    capacity = 2 * mortars // devices
    per = LANES // capacity
    groups = devices // per
    slots = devices * capacity
    blocks = rows * n_frac
    tiles_all = rows * tiles_row
    lines_mv = tiles_all + rows
    share = blocks // devices
    sweeps = OUTER * SWEEPS
    f32, i32 = jnp.float32, jnp.int32
    me = lax.axis_index("frac")
    me_mat = lax.axis_index("mat")
    me_dev = me_mat * n_frac + me
    everyone = [(c, k) for c in range(n_mat) for k in range(n_frac) if c or k]

    barrier = pltpu.get_barrier_semaphore()
    for c, k in everyone:
        pl.semaphore_signal(
            barrier,
            inc=1,
            device_id={"mat": lax.rem(me_mat + c, n_mat), "frac": lax.rem(me + k, n_frac)},
            device_id_type=MESH,
        )

    def load(index, src, dst):
        copy = pltpu.make_async_copy(src, dst, local_sem.at[index])
        copy.start()
        return copy

    press_copy = load(0, press_hbm, grid_ref.at[0, pl.ds(1, width_x)])
    tx_copy = load(1, face_hbm.at[0], tx_ref.at[pl.ds(1, width_x)])
    ty_copy = load(2, face_hbm.at[1], ty_ref)
    tiles_copy = load(3, tiles_hbm, tiles_ref)
    tz_copy = load(4, face_hbm.at[2], tz_ref)
    cell_copy = load(5, cell_hbm, cell_ref)
    msource_copy = load(6, msource_hbm, msource_ref)

    sent = []

    def send(src, dst, send_sem, recv_sem, device):
        copy = pltpu.make_async_remote_copy(
            src_ref=src, dst_ref=dst, send_sem=send_sem, recv_sem=recv_sem, device_id=device, device_id_type=MESH
        )
        copy.start()
        return copy

    def take(ref, sem):
        pltpu.make_async_copy(ref, ref, sem).wait()

    def spread_to_all(source, landing, send_sem, recv_sem):
        for c, k in everyone:
            mat, frac = lax.rem(me_mat + c, n_mat), lax.rem(me + k, n_frac)
            send(source(mat * n_frac + frac), landing.at[me_dev], send_sem, recv_sem, {"mat": mat, "frac": frac})
        sent.append((landing.at[pl.ds(0, devices - 1)], send_sem))

    def spread_to_frac(source, landing, send_sem, recv_sem):
        for k in range(1, n_frac):
            send(source, landing.at[me], send_sem, recv_sem, {"frac": lax.rem(me + k, n_frac)})
        sent.append((landing.at[pl.ds(0, n_frac - 1)], send_sem))

    owner = owner_ref[...]
    named = lax.broadcasted_iota(i32, (devices, mortars), 0) == owner
    named_hot = as_hot(named)
    before = as_hot(lax.broadcasted_iota(i32, (mortars, mortars), 0) <= lax.broadcasted_iota(i32, (mortars, mortars), 1))
    counts = dot_nn(named_hot, before)
    rank = jnp.sum(jnp.where(named, counts, 0.0), axis=0, keepdims=True).astype(i32) - 1
    spot = lax.broadcasted_iota(i32, (LANES, mortars), 0)
    word = lax.rem(spot // capacity + (per - lax.rem(me_dev, per)), per)
    payload = jnp.where(word == 0, cells_ref[...].astype(f32), jnp.where(word == 1, places_ref[...].astype(f32), kappa_in_ref[...]))
    payload = jnp.where((word < 3) & (lax.rem(spot, capacity) == rank), payload, 0.0)
    outgoing = sum(dot_nt(named_hot, part) for part in split_parts(payload, 3))
    mort_out_ref[...] = outgoing.reshape(devices, 1, LANES)

    lane_line = lax.broadcasted_iota(i32, (1, LANES), 1)
    target_row = jnp.where((lane_line >= tiles_all) & (lane_line < lines_mv), me * rows + lane_line - tiles_all, -1)
    for r in range(rows):
        for t in range(tiles_row):
            target_row = jnp.where(lane_line == r * tiles_row + t, cols_ref[t, r], target_row)
    dest_out_ref[...] = target_row.astype(f32)

    pl.semaphore_wait(barrier, devices - 1)
    spread_to_all(lambda target: mort_out_ref.at[target], mort_in_ref, mort_send, mort_recv)
    mort_in_ref[me_dev] = mort_out_ref[me_dev]
    spread_to_frac(begin_ref, vec_ref.at[0], vec_send.at[0], vec_recv.at[0])
    spread_to_frac(dest_out_ref, dest_in_ref, vec_send.at[3], vec_recv.at[3])
    vec_ref[0, me] = begin_ref[...]
    dest_in_ref[me] = dest_out_ref[...]

    lanes = lax.broadcasted_iota(i32, (width_y, depth_z), 1)
    lines = lax.broadcasted_iota(i32, (width_y, depth_z), 0)
    next_mat, prev_mat = lax.rem(me_mat + 1, n_mat), lax.rem(me_mat + n_mat - 1, n_mat)
    next_frac, prev_frac = lax.rem(me + 1, n_frac), lax.rem(me + n_frac - 1, n_frac)
    halos = {}
    slow_sends = []

    def send_halo(sweep):
        sems = [(halo_send.at[sweep, d], halo_recv.at[sweep, d]) for d in range(4)]
        halos[sweep] = [
            send(grid_ref.at[sweep, width_x], grid_ref.at[sweep, 0], *sems[0], {"mat": next_mat}),
            send(grid_ref.at[sweep, 1], grid_ref.at[sweep, width_x + 1], *sems[1], {"mat": prev_mat}),
            send(edge_ref.at[sweep, 0], side_ref.at[sweep, 0], *sems[2], {"frac": next_frac}),
            send(edge_ref.at[sweep, 1], side_ref.at[sweep, 1], *sems[3], {"frac": prev_frac}),
        ]
        slow_sends.extend(halos[sweep])

    def wait_halo(sweep):
        for copy in halos[sweep]:
            copy.wait_recv()
        grid_ref[sweep, 0] = jnp.where(me_mat == 0, 0.0, grid_ref[sweep, 0])
        grid_ref[sweep, width_x + 1] = jnp.where(me_mat == n_mat - 1, 0.0, grid_ref[sweep, width_x + 1])
        side_ref[sweep, 0] = jnp.where(me == 0, 0.0, side_ref[sweep, 0])
        side_ref[sweep, 1] = jnp.where(me == n_frac - 1, 0.0, side_ref[sweep, 1])

    press_copy.wait()
    edge_ref[0, 0] = grid_ref[0, 1 : width_x + 1, width_y - 1, :]
    edge_ref[0, 1] = grid_ref[0, 1 : width_x + 1, 0, :]
    send_halo(0)
    tx_copy.wait()
    ty_copy.wait()
    ty_edge_ref[...] = ty_ref[:, width_y - 1, :]
    coef_copies = [
        send(tx_ref.at[width_x], tx_ref.at[0], halo_send.at[sweeps, 0], halo_recv.at[sweeps, 0], {"mat": next_mat}),
        send(ty_edge_ref, ty_side_ref, halo_send.at[sweeps, 2], halo_recv.at[sweeps, 2], {"frac": next_frac}),
    ]
    slow_sends.extend(coef_copies)
    spread_to_frac(fsource_ref, vec_ref.at[1], vec_send.at[1], vec_recv.at[1])
    spread_to_frac(diag_ref, vec_ref.at[2], vec_send.at[2], vec_recv.at[2])
    vec_ref[1, me] = fsource_ref[...]
    vec_ref[2, me] = diag_ref[...]

    def gathered(index):
        take(vec_ref.at[index, pl.ds(0, n_frac - 1)], vec_recv.at[index])
        return vec_ref[index].reshape(blocks, size_b)

    def set_parts(sweep):
        high, low = split_parts(grid_ref[sweep, 1 : width_x + 1].reshape(grid_rows, depth_z), 2)
        parts_ref[0] = high
        parts_ref[1] = low

    def set_inverse():
        tz_copy.wait()
        cell_copy.wait()
        for copy in coef_copies:
            copy.wait_recv()
        tx_ref[0] = jnp.where(me_mat == 0, 0.0, tx_ref[0])
        ty_side_ref[...] = jnp.where(me == 0, 0.0, ty_side_ref[...])

        def plane(x, carry):
            ty_here, tz_here = ty_ref[x], tz_ref[x]
            tz_in = jnp.where(lanes == depth_z - 1, 0.0, tz_here)
            ty_low = jnp.where(lines == 0, ty_side_ref[pl.ds(x, 1), :], pltpu.roll(ty_here, 1, 0))
            tz_low = pltpu.roll(tz_in, 1, 1)
            inv_ref[x] = relax_weight / (cell_ref[x] + tx_ref[x + 1] + tx_ref[x] + ty_here + ty_low + tz_here + tz_low)
            tz_ref[x] = tz_in
            return carry

        lax.fori_loop(0, width_x, plane, 0)

    def sweep_part(sweep, low, high):
        def plane(x, carry):
            here = grid_ref[sweep, x + 1]
            ty_here, tz_here = ty_ref[x], tz_ref[x]
            up = jnp.where(lines == width_y - 1, side_ref[sweep, 1, pl.ds(x, 1), :], pltpu.roll(here, width_y - 1, 0))
            down = jnp.where(
                lines == 0,
                ty_side_ref[pl.ds(x, 1), :] * side_ref[sweep, 0, pl.ds(x, 1), :],
                pltpu.roll(ty_here * here, 1, 0),
            )
            total = base_ref[x] + tx_ref[x + 1] * grid_ref[sweep, x + 2] + tx_ref[x] * grid_ref[sweep, x]
            total = total + ty_here * up + down
            total = total + tz_here * pltpu.roll(here, depth_z - 1, 1) + pltpu.roll(tz_here * here, 1, 1)
            value = (1.0 - relax_weight) * here + inv_ref[x] * total
            if sweep + 1 < sweeps:
                grid_ref[sweep + 1, x + 1] = value
                edge_ref[sweep + 1, 0, pl.ds(x, 1), :] = value[width_y - 1 :]
                edge_ref[sweep + 1, 1, pl.ds(x, 1), :] = value[:1]
            else:
                out_ref[x] = value
            return carry

        lax.fori_loop(low, high, plane, 0)

    set_parts(0)

    take(mort_in_ref.at[pl.ds(0, devices - 1)], mort_recv)
    arrived = mort_in_ref[...].reshape(devices, LANES)
    window = lax.broadcasted_iota(i32, (devices, LANES), 1) // capacity
    device = lax.broadcasted_iota(i32, (devices, LANES), 0)

    def slot_line(word_no):
        turned = pltpu.roll(arrived, LANES - word_no * capacity, 1) if word_no else arrived
        chosen = jnp.where(lax.rem(device, per) == window, turned, 0.0)
        return jnp.concatenate(
            [jnp.sum(chosen[g * per : (g + 1) * per], axis=0, keepdims=True) for g in range(groups)], axis=1
        )

    cell = slot_line(0).astype(i32)
    place = slot_line(1).astype(i32)
    kappa = slot_line(2)
    cell_row = cell // depth_z
    cell_lane = cell - cell_row * depth_z
    block_of = place // size_b
    lane_of = place - block_of * size_b
    lane_hot_ref[...] = as_hot(lax.broadcasted_iota(i32, (depth_z, slots), 0) == cell_lane)
    by_lane = as_hot(lax.broadcasted_iota(i32, (size_b, slots), 0) == lane_of)
    by_block = lax.broadcasted_iota(i32, (blocks, slots), 0) == block_of

    quarter = slots // 4
    grid_line = lax.broadcasted_iota(i32, (grid_rows, quarter), 0)

    def traces():
        found = []
        for q in range(4):
            hot = lane_hot_ref[:, q * quarter : (q + 1) * quarter]
            picked = dot_nn(parts_ref[0], hot) + dot_nn(parts_ref[1], hot)
            found.append(
                jnp.sum(jnp.where(grid_line == cell_row[:, q * quarter : (q + 1) * quarter], picked, 0.0), axis=0, keepdims=True)
            )
        return jnp.concatenate(found, axis=1)

    def at_slots(values):
        picked = sum(dot_nn(part, by_lane) for part in split_parts(values, 3))
        return jnp.sum(jnp.where(by_block, picked, 0.0), axis=0, keepdims=True)

    def landed(values):
        return sum(dot_nt(as_part, by_lane) for as_part in split_parts(jnp.where(by_block, values, 0.0), 3))

    shares = [(rs_out_0, rs_in_0, ag_0), (rs_out_1, rs_in_1, ag_1)]

    def scatter_share(stage, arrays):
        out, landing, _ = shares[stage]
        for n, array in enumerate(arrays):
            out[:, n] = array.reshape(devices, share, size_b)
        spread_to_all(lambda target: out.at[target], landing, rs_send.at[stage], rs_recv.at[stage])
        landing[me_dev] = out[me_dev]

    def gather_share(stage):
        _, landing, whole = shares[stage]
        take(landing.at[pl.ds(0, devices - 1)], rs_recv.at[stage])
        mine = landing[0]
        for d in range(1, devices):
            mine = mine + landing[d]
        whole[me_dev] = mine
        spread_to_all(lambda target: whole.at[me_dev], whole, ag_send.at[stage], ag_recv.at[stage])

    def whole_shares(stage):
        _, _, whole = shares[stage]
        take(whole.at[pl.ds(0, devices - 1)], ag_recv.at[stage])
        return [whole[:, n].reshape(blocks, size_b) for n in range(whole.shape[1])]

    half = tiles_all // 2

    def send_lines(phase, low, high):
        part = pl.ds(low, high - low)
        for k in range(1, n_frac):
            send(
                mv_ref.at[phase, me, part],
                mv_ref.at[phase, me, part],
                mv_send.at[phase],
                mv_recv.at[phase],
                {"frac": lax.rem(me + k, n_frac)},
            )

    def products(phase, with_back):
        own = vector_ref[phase, pl.ds(pl.multiple_of(me * rows, rows), rows), :]
        for r in range(rows):
            down = jnp.broadcast_to(own[r : r + 1], (size_b, size_b)).T
            total = None
            for t in range(tiles_row):
                tile = tiles_ref[r, t]
                part = tile * vector_ref[phase, pl.ds(cols_ref[t, r], 1), :]
                total = part if total is None else total + part
                if with_back:
                    line = r * tiles_row + t
                    mv_ref[phase, me, line : line + 1, :] = jnp.sum(tile * down, axis=0, keepdims=True)
            mv_ref[phase, me, tiles_all + r : tiles_all + r + 1, :] = jnp.sum(total.T, axis=0, keepdims=True)
            if with_back and (r + 1) * tiles_row == half:
                send_lines(phase, 0, half)

    def start_matvec(phase, vector):
        vector_ref[phase] = vector
        products(phase, True)
        send_lines(phase, half, lines_mv)
        sent.append((mv_ref.at[phase, pl.ds(0, n_frac - 1)], mv_send.at[phase]))

    def finish_matvec(phase, vector):
        take(mv_ref.at[phase, pl.ds(0, n_frac - 1)], mv_recv.at[phase])
        forward = mv_ref[phase, :, tiles_all:].reshape(blocks, size_b)
        product = total_of(vector * (diag * vector + forward))
        arrived = mv_ref[phase].reshape(n_frac * lines_mv, size_b)
        both = sum(dot_nn(targets, part) for part in split_parts(arrived, 2))
        return product, diag * vector + 0.5 * both

    def set_row_hot():
        line = lax.broadcasted_iota(i32, (grid_rows, quarter), 0)
        for q in range(4):
            cut = slice(q * quarter, (q + 1) * quarter)
            row_hot_ref[:, cut] = as_hot(line == cell_row[:, cut])

    part_x = width_x // 4

    def set_sources(flux):
        wide = lane_hot_ref[...]
        weights = [wide * part for part in split_parts(flux, 2)]
        for q in range(4):
            low = q * part_x
            hot = row_hot_ref[low * width_y : (low + part_x) * width_y, :]
            total = sum(dot_nt(hot, weight) for weight in weights)
            base_ref[low : low + part_x] = msource_ref[low : low + part_x] + total.reshape(part_x, width_y, depth_z)

    begin = gathered(0)
    trace = traces()
    flux = kappa * (trace - at_slots(begin))
    scatter_share(0, [landed(flux)])

    tiles_copy.wait()
    start_matvec(0, begin)
    set_inverse()
    set_row_hot()
    msource_copy.wait()
    set_sources(flux)
    take(dest_in_ref.at[pl.ds(0, n_frac - 1)], vec_recv.at[3])
    block_line = lax.broadcasted_iota(i32, (blocks, LANES), 0)
    targets = jnp.concatenate(
        [as_hot(block_line == dest_in_ref[d].astype(i32))[:, :lines_mv] for d in range(n_frac)], axis=1
    )
    fsource = gathered(1)
    diag = gathered(2)
    gather_share(0)

    wait_halo(0)
    sweep_part(0, 0, width_x)
    send_halo(1)
    _, image = finish_matvec(0, begin)
    (loaded,) = whole_shares(0)
    residual = fsource + loaded - image
    fracture = begin

    def fill(number):
        if number == 0:
            wait_halo(1)
            sweep_part(1, 0, width_x)
            send_halo(2)
            set_parts(2)
            state["trace"] = traces()
            scatter_share(1, [landed(kappa * state["trace"]), landed(kappa)])
        elif number == 2:
            gather_share(1)
        elif number == 3:
            flux = kappa * (state["trace"] - at_slots(state["fracture"]))
            for g in range(groups):
                back_out_ref[g] = flux[:, g * LANES : (g + 1) * LANES]
            spread_to_all(lambda target: back_out_ref.at[target // per], back_in_ref, back_send, back_recv)
            back_in_ref[me_dev] = back_out_ref[me_dev // per]
            set_sources(flux)
            wait_halo(2)
            sweep_part(2, 0, width_x)
            send_halo(3)
        elif number == 4:
            wait_halo(3)
            sweep_part(3, 0, width_x)
        elif number == 5:
            take(back_in_ref.at[pl.ds(0, devices - 1)], back_recv)
            came = back_in_ref[...].reshape(devices, LANES)
            lines_back = sum(
                lax.dot_general(part, named_hot, (((0,), (0,)), ((), ())), preferred_element_type=f32)
                for part in split_parts(came, 3)
            )
            want = rank + capacity * lax.rem(me_dev, per)
            flux_out_ref[...] = jnp.sum(jnp.where(spot == want, lines_back, 0.0), axis=0, keepdims=True)

    state = {}
    last = OUTER * CG_ITERS - 1
    for number in range(OUTER * CG_ITERS):
        step = number % CG_ITERS
        phase = number + 1
        if number == CG_ITERS:
            traced, weight = whole_shares(1)
            residual = residual + ((traced - weight * fracture) - loaded)
            state["fracture"] = fracture
        if number < last:
            start_matvec(phase, residual)
        else:
            vector_ref[phase] = residual
            products(phase, False)
            mine = pl.ds(pl.multiple_of(me * rows, rows), rows)
            part_out_ref[...] = jnp.sum(
                vector_ref[phase, mine, :] * mv_ref[phase, me, tiles_all:, :], axis=0, keepdims=True
            )
            spread_to_frac(part_out_ref, part_in_ref, part_send, part_recv)
            part_in_ref[me] = part_out_ref[...]
        norm_next = total_of(residual * residual)
        fill(number)
        if number < last:
            product, image = finish_matvec(phase, residual)
        else:
            take(part_in_ref.at[pl.ds(0, n_frac - 1)], part_recv)
            product = total_of(diag * residual * residual)
            lines_all = part_in_ref[0]
            for d in range(1, n_frac):
                lines_all = lines_all + part_in_ref[d]
            product = product + total_of(lines_all)
        if step == 0:
            alpha = norm_next / product
            direction = residual
            along = image
        else:
            ratio = norm_next / norm_now
            alpha = norm_next / (product - ratio * norm_next / alpha)
            direction = residual + ratio * direction
            if number < last:
                along = image + ratio * along
        norm_now = norm_next
        fracture = fracture + alpha * direction
        if number < last:
            residual = residual - alpha * along

    vector_ref[0] = fracture
    own_ref[...] = vector_ref[0, pl.ds(pl.multiple_of(me * rows, rows), rows), :]
    for ref, sem in sent:
        take(ref, sem)
    for copy in slow_sends:
        copy.wait_send()


def coupled(pressure, face, cell_coef, matrix_source, tiles, owner, cells, places, kappa, tile_cols, diag, begin, fsource):
    n_frac, n_mat = lax.axis_size("frac"), lax.axis_size("mat")
    devices = n_frac * n_mat
    rows, tiles_row, size_b = tiles.shape[0], tiles.shape[1], tiles.shape[3]
    blocks = rows * n_frac
    x, y, z = pressure.shape
    mortars = owner.shape[1]
    capacity = 2 * mortars // devices
    slots = devices * capacity
    groups = slots // LANES
    share = blocks // devices
    lines_mv = rows * tiles_row + rows
    f32, bf16 = jnp.float32, jnp.bfloat16
    vmem = pl.BlockSpec(memory_space=pltpu.VMEM)
    smem = pl.BlockSpec(memory_space=pltpu.SMEM)
    hbm = pl.BlockSpec(memory_space=pltpu.HBM)
    phases = OUTER * CG_ITERS + 1
    sweeps = OUTER * SWEEPS
    dma = pltpu.SemaphoreType.DMA
    return pl.pallas_call(
        functools.partial(coupled_kernel, n_frac, n_mat),
        out_shape=(
            pltpu.VMEM((x, y, z), f32),
            pltpu.VMEM((rows, size_b), f32),
            pltpu.VMEM((1, mortars), f32),
        ),
        in_specs=[hbm] * 5 + [vmem] * 4 + [smem] + [vmem] * 3,
        out_specs=(vmem, vmem, vmem),
        scratch_shapes=[
            pltpu.VMEM((sweeps, x + 2, y, z), f32),
            pltpu.VMEM((x + 1, y, z), f32),
            pltpu.VMEM((x, y, z), f32),
            pltpu.VMEM((x, y, z), f32),
            pltpu.VMEM((x, y, z), f32),
            pltpu.VMEM((x, y, z), f32),
            pltpu.VMEM((x, y, z), f32),
            pltpu.VMEM((x, y, z), f32),
            pltpu.VMEM((rows, tiles_row, size_b, size_b), f32),
            pltpu.VMEM((2, x * y, z), bf16),
            pltpu.VMEM((x * y, slots), bf16),
            pltpu.VMEM((z, slots), bf16),
            pltpu.VMEM((sweeps, 2, x, z), f32),
            pltpu.VMEM((sweeps, 2, x, z), f32),
            pltpu.VMEM((x, z), f32),
            pltpu.VMEM((x, z), f32),
            pltpu.VMEM((devices, 1, LANES), f32),
            pltpu.VMEM((devices, 1, LANES), f32),
            pltpu.VMEM((3, n_frac, rows, size_b), f32),
            pltpu.VMEM((1, LANES), f32),
            pltpu.VMEM((n_frac, 1, LANES), f32),
            pltpu.VMEM((phases, n_frac, lines_mv, size_b), f32),
            pltpu.VMEM((phases, blocks, size_b), f32),
            pltpu.VMEM((devices, 1, share, size_b), f32),
            pltpu.VMEM((devices, 1, share, size_b), f32),
            pltpu.VMEM((devices, 1, share, size_b), f32),
            pltpu.VMEM((devices, 2, share, size_b), f32),
            pltpu.VMEM((devices, 2, share, size_b), f32),
            pltpu.VMEM((devices, 2, share, size_b), f32),
            pltpu.VMEM((1, size_b), f32),
            pltpu.VMEM((n_frac, 1, size_b), f32),
            pltpu.VMEM((groups, 1, LANES), f32),
            pltpu.VMEM((devices, 1, LANES), f32),
            dma((7,)),
            dma,
            dma,
            dma((4,)),
            dma((4,)),
            dma((phases,)),
            dma((phases,)),
            dma((2,)),
            dma((2,)),
            dma((2,)),
            dma((2,)),
            dma,
            dma,
            dma,
            dma,
            dma((sweeps + 1, 4)),
            dma((sweeps + 1, 4)),
        ],
        compiler_params=pltpu.CompilerParams(
            collective_id=0, has_side_effects=True, vmem_limit_bytes=60 * 1024 * 1024
        ),
        name="coupled",
    )(pressure, face, cell_coef, matrix_source, tiles, owner, cells, places, kappa, tile_cols, diag, begin, fsource)


def body(
    pressure_start,
    face_trans,
    cell_coef,
    matrix_source,
    mortar_owner,
    mortar_cell,
    mortar_frac,
    mortar_kappa,
    tiles,
    tile_cols,
    frac_diag,
    frac_source,
    fracture_start,
):
    size_b = tiles.shape[2]
    line = (1, -1)
    blocked = (-1, size_b)
    pressure, fracture, flux = coupled(
        pressure_start,
        face_trans,
        cell_coef,
        matrix_source,
        tiles,
        mortar_owner.reshape(line),
        mortar_cell.reshape(line),
        mortar_frac.reshape(line),
        mortar_kappa.reshape(line),
        tile_cols.T,
        frac_diag.reshape(blocked),
        fracture_start.reshape(blocked),
        frac_source.reshape(blocked),
    )
    return (pressure, fracture.reshape(-1), flux.reshape(-1))


def solution(mesh):
    in_specs = (
        P("mat", "frac", None),
        P(None, "mat", "frac", None),
        P("mat", "frac", None),
        P("mat", "frac", None),
        P(("mat", "frac"), None),
        P(("mat", "frac")),
        P(("mat", "frac")),
        P(("mat", "frac")),
        P("frac", None, None, None),
        P("frac", None),
        P("frac"),
        P("frac"),
        P("frac"),
    )
    out_specs = (P("mat", "frac", None), P("frac"), P(("mat", "frac")))
    return jax.shard_map(body, mesh=mesh, in_specs=in_specs, out_specs=out_specs, check_vma=False)
```

```python
import functools

import jax
import jax.numpy as jnp
from jax import lax
from jax.experimental import pallas as pl
from jax.experimental.pallas import tpu as pltpu
from jax.sharding import PartitionSpec as P

SWEEPS = 2
CG_ITERS = 3
OUTER = 2

MESH = pl.DeviceIdType.MESH
LANES = 128

relax_weight = 0.8


def split_parts(values, count):
    parts = []
    for _ in range(count - 1):
        part = values.astype(jnp.bfloat16)
        parts.append(part)
        values = values - part.astype(jnp.float32)
    parts.append(values.astype(jnp.bfloat16))
    return parts


def as_hot(mask):
    return mask.astype(jnp.float32).astype(jnp.bfloat16)


def dot_nn(a, b):
    return lax.dot_general(a, b, (((1,), (0,)), ((), ())), preferred_element_type=jnp.float32)


def dot_nt(a, b):
    return lax.dot_general(a, b, (((1,), (1,)), ((), ())), preferred_element_type=jnp.float32)


def total_of(values):
    return jnp.sum(values, axis=(0, 1), keepdims=True)


def coupled_kernel(n_frac, n_mat, *refs):
    (press_hbm, face_hbm, cell_hbm, msource_hbm, tiles_hbm, owner_ref, cells_ref, places_ref, kappa_in_ref, cols_ref,
     diag_ref, begin_ref, fsource_ref, out_ref, own_ref, flux_out_ref, *scratch) = refs
    (grid_ref, tx_ref, ty_ref, tz_ref, inv_ref, cell_ref, msource_ref, base_ref, tiles_ref, parts_ref,
     row_hot_ref, lane_hot_ref, side_ref, edge_ref, ty_edge_ref, ty_side_ref, mort_out_ref, mort_in_ref, vec_ref,
     dest_out_ref, dest_in_ref, mv_ref, vector_ref, rs_out_0, rs_in_0, ag_0, rs_out_1, rs_in_1, ag_1, part_out_ref, part_in_ref,
     back_out_ref, back_in_ref, local_sem, mort_send, mort_recv, vec_send, vec_recv, mv_send, mv_recv,
     pair_recv, rs_send, rs_recv, ag_send, ag_recv, part_send, part_recv, back_send, back_recv, halo_send, halo_recv) = scratch
    rows, tiles_row, size_b = tiles_ref.shape[0], tiles_ref.shape[1], tiles_ref.shape[3]
    width_x, width_y, depth_z = inv_ref.shape
    grid_rows = width_x * width_y
    mortars = owner_ref.shape[1]
    devices = n_mat * n_frac
    capacity = 2 * mortars // devices
    per = LANES // capacity
    groups = devices // per
    slots = devices * capacity
    blocks = rows * n_frac
    half = rows // 2
    lines_half = half * tiles_row + half
    stride = -(-lines_half // 8) * 8
    share = blocks // devices
    sweeps = OUTER * SWEEPS
    f32, i32 = jnp.float32, jnp.int32
    me = lax.axis_index("frac")
    me_mat = lax.axis_index("mat")
    me_dev = me_mat * n_frac + me
    core = lax.rem(me_mat, 2)
    sibling = me_mat + 1 - 2 * core
    everyone = [(c, k) for c in range(n_mat) for k in range(n_frac) if c or k]

    barrier = pltpu.get_barrier_semaphore()
    for c, k in everyone:
        pl.semaphore_signal(
            barrier,
            inc=1,
            device_id={"mat": lax.rem(me_mat + c, n_mat), "frac": lax.rem(me + k, n_frac)},
            device_id_type=MESH,
        )

    def load(index, src, dst):
        copy = pltpu.make_async_copy(src, dst, local_sem.at[index])
        copy.start()
        return copy

    press_copy = load(0, press_hbm, grid_ref.at[0, pl.ds(1, width_x)])
    tx_copy = load(1, face_hbm.at[0], tx_ref.at[pl.ds(1, width_x)])
    ty_copy = load(2, face_hbm.at[1], ty_ref)
    tiles_copy = load(3, tiles_hbm, tiles_ref)
    tz_copy = load(4, face_hbm.at[2], tz_ref)
    cell_copy = load(5, cell_hbm, cell_ref)
    msource_copy = load(6, msource_hbm, msource_ref)

    sent = []

    def send(src, dst, send_sem, recv_sem, device):
        copy = pltpu.make_async_remote_copy(
            src_ref=src, dst_ref=dst, send_sem=send_sem, recv_sem=recv_sem, device_id=device, device_id_type=MESH
        )
        copy.start()
        return copy

    def take(ref, sem):
        pltpu.make_async_copy(ref, ref, sem).wait()

    def spread_to_all(source, landing, send_sem, recv_sem):
        for c, k in everyone:
            mat, frac = lax.rem(me_mat + c, n_mat), lax.rem(me + k, n_frac)
            send(source(mat * n_frac + frac), landing.at[me_dev], send_sem, recv_sem, {"mat": mat, "frac": frac})
        sent.append((landing.at[pl.ds(0, devices - 1)], send_sem))

    def spread_to_frac(source, landing, send_sem, recv_sem):
        for k in range(1, n_frac):
            send(source, landing.at[me], send_sem, recv_sem, {"frac": lax.rem(me + k, n_frac)})
        sent.append((landing.at[pl.ds(0, n_frac - 1)], send_sem))

    owner = owner_ref[...]
    named = lax.broadcasted_iota(i32, (devices, mortars), 0) == owner
    named_hot = as_hot(named)
    before = as_hot(lax.broadcasted_iota(i32, (mortars, mortars), 0) <= lax.broadcasted_iota(i32, (mortars, mortars), 1))
    counts = dot_nn(named_hot, before)
    rank = jnp.sum(jnp.where(named, counts, 0.0), axis=0, keepdims=True).astype(i32) - 1
    spot = lax.broadcasted_iota(i32, (LANES, mortars), 0)
    word = lax.rem(spot // capacity + (per - lax.rem(me_dev, per)), per)
    payload = jnp.where(word == 0, cells_ref[...].astype(f32), jnp.where(word == 1, places_ref[...].astype(f32), kappa_in_ref[...]))
    payload = jnp.where((word < 3) & (lax.rem(spot, capacity) == rank), payload, 0.0)
    outgoing = sum(dot_nt(named_hot, part) for part in split_parts(payload, 3))
    mort_out_ref[...] = outgoing.reshape(devices, 1, LANES)

    lane_line = lax.broadcasted_iota(i32, (1, LANES), 1)
    target_row = jnp.full((1, LANES), -1, i32)
    for h in range(2):
        for n in range(lines_half):
            r, t = h * half + n // tiles_row, n % tiles_row
            block = cols_ref[t, r] if n < half * tiles_row else me * rows + h * half + n - half * tiles_row
            target_row = jnp.where(lane_line == h * stride + n, block, target_row)
    dest_out_ref[...] = target_row.astype(f32)

    if stride > lines_half:
        mv_ref[:, :, :, lines_half:, :] = jnp.zeros((mv_ref.shape[0], n_frac, 2, stride - lines_half, size_b), f32)

    pl.semaphore_wait(barrier, devices - 1)
    spread_to_all(lambda target: mort_out_ref.at[target], mort_in_ref, mort_send, mort_recv)
    mort_in_ref[me_dev] = mort_out_ref[me_dev]
    spread_to_frac(begin_ref, vec_ref.at[0], vec_send.at[0], vec_recv.at[0])
    spread_to_frac(dest_out_ref, dest_in_ref, vec_send.at[3], vec_recv.at[3])
    vec_ref[0, me] = begin_ref[...]
    dest_in_ref[me] = dest_out_ref[...]

    lanes = lax.broadcasted_iota(i32, (width_y, depth_z), 1)
    lines = lax.broadcasted_iota(i32, (width_y, depth_z), 0)
    next_mat, prev_mat = lax.rem(me_mat + 1, n_mat), lax.rem(me_mat + n_mat - 1, n_mat)
    next_frac, prev_frac = lax.rem(me + 1, n_frac), lax.rem(me + n_frac - 1, n_frac)
    halos = {}
    slow_sends = []

    def send_halo(sweep):
        sems = [(halo_send.at[sweep, d], halo_recv.at[sweep, d]) for d in range(4)]
        halos[sweep] = [
            send(grid_ref.at[sweep, width_x], grid_ref.at[sweep, 0], *sems[0], {"mat": next_mat}),
            send(grid_ref.at[sweep, 1], grid_ref.at[sweep, width_x + 1], *sems[1], {"mat": prev_mat}),
            send(edge_ref.at[sweep, 0], side_ref.at[sweep, 0], *sems[2], {"frac": next_frac}),
            send(edge_ref.at[sweep, 1], side_ref.at[sweep, 1], *sems[3], {"frac": prev_frac}),
        ]
        slow_sends.extend(halos[sweep])

    def wait_halo(sweep):
        for copy in halos[sweep]:
            copy.wait_recv()
        grid_ref[sweep, 0] = jnp.where(me_mat == 0, 0.0, grid_ref[sweep, 0])
        grid_ref[sweep, width_x + 1] = jnp.where(me_mat == n_mat - 1, 0.0, grid_ref[sweep, width_x + 1])
        side_ref[sweep, 0] = jnp.where(me == 0, 0.0, side_ref[sweep, 0])
        side_ref[sweep, 1] = jnp.where(me == n_frac - 1, 0.0, side_ref[sweep, 1])

    press_copy.wait()
    edge_ref[0, 0] = grid_ref[0, 1 : width_x + 1, width_y - 1, :]
    edge_ref[0, 1] = grid_ref[0, 1 : width_x + 1, 0, :]
    send_halo(0)
    tx_copy.wait()
    ty_copy.wait()
    ty_edge_ref[...] = ty_ref[:, width_y - 1, :]
    coef_copies = [
        send(tx_ref.at[width_x], tx_ref.at[0], halo_send.at[sweeps, 0], halo_recv.at[sweeps, 0], {"mat": next_mat}),
        send(ty_edge_ref, ty_side_ref, halo_send.at[sweeps, 2], halo_recv.at[sweeps, 2], {"frac": next_frac}),
    ]
    slow_sends.extend(coef_copies)
    spread_to_frac(fsource_ref, vec_ref.at[1], vec_send.at[1], vec_recv.at[1])
    spread_to_frac(diag_ref, vec_ref.at[2], vec_send.at[2], vec_recv.at[2])
    vec_ref[1, me] = fsource_ref[...]
    vec_ref[2, me] = diag_ref[...]

    def gathered(index):
        take(vec_ref.at[index, pl.ds(0, n_frac - 1)], vec_recv.at[index])
        return vec_ref[index].reshape(blocks, size_b)

    def set_parts(sweep):
        high, low = split_parts(grid_ref[sweep, 1 : width_x + 1].reshape(grid_rows, depth_z), 2)
        parts_ref[0] = high
        parts_ref[1] = low

    def set_inverse():
        tz_copy.wait()
        cell_copy.wait()
        for copy in coef_copies:
            copy.wait_recv()
        tx_ref[0] = jnp.where(me_mat == 0, 0.0, tx_ref[0])
        ty_side_ref[...] = jnp.where(me == 0, 0.0, ty_side_ref[...])

        def plane(x, carry):
            ty_here, tz_here = ty_ref[x], tz_ref[x]
            tz_in = jnp.where(lanes == depth_z - 1, 0.0, tz_here)
            ty_low = jnp.where(lines == 0, ty_side_ref[pl.ds(x, 1), :], pltpu.roll(ty_here, 1, 0))
            tz_low = pltpu.roll(tz_in, 1, 1)
            inv_ref[x] = relax_weight / (cell_ref[x] + tx_ref[x + 1] + tx_ref[x] + ty_here + ty_low + tz_here + tz_low)
            tz_ref[x] = tz_in
            return carry

        lax.fori_loop(0, width_x, plane, 0)

    def sweep_part(sweep, low, high):
        def plane(x, carry):
            here = grid_ref[sweep, x + 1]
            ty_here, tz_here = ty_ref[x], tz_ref[x]
            up = jnp.where(lines == width_y - 1, side_ref[sweep, 1, pl.ds(x, 1), :], pltpu.roll(here, width_y - 1, 0))
            down = jnp.where(
                lines == 0,
                ty_side_ref[pl.ds(x, 1), :] * side_ref[sweep, 0, pl.ds(x, 1), :],
                pltpu.roll(ty_here * here, 1, 0),
            )
            total = base_ref[x] + tx_ref[x + 1] * grid_ref[sweep, x + 2] + tx_ref[x] * grid_ref[sweep, x]
            total = total + ty_here * up + down
            total = total + tz_here * pltpu.roll(here, depth_z - 1, 1) + pltpu.roll(tz_here * here, 1, 1)
            value = (1.0 - relax_weight) * here + inv_ref[x] * total
            if sweep + 1 < sweeps:
                grid_ref[sweep + 1, x + 1] = value
                edge_ref[sweep + 1, 0, pl.ds(x, 1), :] = value[width_y - 1 :]
                edge_ref[sweep + 1, 1, pl.ds(x, 1), :] = value[:1]
            else:
                out_ref[x] = value
            return carry

        lax.fori_loop(low, high, plane, 0)

    set_parts(0)

    take(mort_in_ref.at[pl.ds(0, devices - 1)], mort_recv)
    arrived = mort_in_ref[...].reshape(devices, LANES)
    window = lax.broadcasted_iota(i32, (devices, LANES), 1) // capacity
    device = lax.broadcasted_iota(i32, (devices, LANES), 0)

    def slot_line(word_no):
        turned = pltpu.roll(arrived, LANES - word_no * capacity, 1) if word_no else arrived
        chosen = jnp.where(lax.rem(device, per) == window, turned, 0.0)
        return jnp.concatenate(
            [jnp.sum(chosen[g * per : (g + 1) * per], axis=0, keepdims=True) for g in range(groups)], axis=1
        )

    cell = slot_line(0).astype(i32)
    place = slot_line(1).astype(i32)
    kappa = slot_line(2)
    cell_row = cell // depth_z
    cell_lane = cell - cell_row * depth_z
    block_of = place // size_b
    lane_of = place - block_of * size_b
    lane_hot_ref[...] = as_hot(lax.broadcasted_iota(i32, (depth_z, slots), 0) == cell_lane)
    by_lane = as_hot(lax.broadcasted_iota(i32, (size_b, slots), 0) == lane_of)
    by_block = lax.broadcasted_iota(i32, (blocks, slots), 0) == block_of

    quarter = slots // 4
    grid_line = lax.broadcasted_iota(i32, (grid_rows, quarter), 0)

    def traces():
        found = []
        for q in range(4):
            hot = lane_hot_ref[:, q * quarter : (q + 1) * quarter]
            picked = dot_nn(parts_ref[0], hot) + dot_nn(parts_ref[1], hot)
            found.append(
                jnp.sum(jnp.where(grid_line == cell_row[:, q * quarter : (q + 1) * quarter], picked, 0.0), axis=0, keepdims=True)
            )
        return jnp.concatenate(found, axis=1)

    def at_slots(values):
        picked = sum(dot_nn(part, by_lane) for part in split_parts(values, 3))
        return jnp.sum(jnp.where(by_block, picked, 0.0), axis=0, keepdims=True)

    def landed(values):
        return sum(dot_nt(as_part, by_lane) for as_part in split_parts(jnp.where(by_block, values, 0.0), 3))

    shares = [(rs_out_0, rs_in_0, ag_0), (rs_out_1, rs_in_1, ag_1)]

    def scatter_share(stage, arrays):
        out, landing, _ = shares[stage]
        for n, array in enumerate(arrays):
            out[:, n] = array.reshape(devices, share, size_b)
        spread_to_all(lambda target: out.at[target], landing, rs_send.at[stage], rs_recv.at[stage])
        landing[me_dev] = out[me_dev]

    def gather_share(stage):
        _, landing, whole = shares[stage]
        take(landing.at[pl.ds(0, devices - 1)], rs_recv.at[stage])
        mine = landing[0]
        for d in range(1, devices):
            mine = mine + landing[d]
        whole[me_dev] = mine
        spread_to_all(lambda target: whole.at[me_dev], whole, ag_send.at[stage], ag_recv.at[stage])

    def whole_shares(stage):
        _, _, whole = shares[stage]
        take(whole.at[pl.ds(0, devices - 1)], ag_recv.at[stage])
        return [whole[:, n].reshape(blocks, size_b) for n in range(whole.shape[1])]

    def tile_line(phase, r, down, place):
        total = None
        for t in range(tiles_row):
            tile = tiles_ref[r, t]
            part = tile * vector_ref[phase, pl.ds(cols_ref[t, r], 1), :]
            total = part if total is None else total + part
            if place is not None:
                line = place * tiles_row + t
                mv_ref[phase, me, core, line : line + 1, :] = jnp.sum(tile * down, axis=0, keepdims=True)
        return jnp.sum(total.T, axis=0, keepdims=True)

    falling = [n_frac - 1 - n - (n_frac - 1 - n <= me).astype(i32) for n in range(n_frac - 1)]
    rising = [n + (n >= me).astype(i32) for n in range(n_frac - 1)]
    near_first = [jnp.where(2 * me < n_frac, up, down) for up, down in zip(rising, falling)]
    lines_sent = pl.ds(0, lines_half)

    def start_matvec(phase, vector):
        vector_ref[phase] = vector
        for n in range(half):
            r = core * half + n
            own = vector_ref[phase, pl.ds(me * rows + r, 1), :]
            forward = tile_line(phase, r, jnp.broadcast_to(own, (size_b, size_b)).T, n)
            line = half * tiles_row + n
            mv_ref[phase, me, core, line : line + 1, :] = forward
        lines = mv_ref.at[phase, me, core, lines_sent]
        for target in reversed(near_first):
            send(lines, lines, mv_send.at[phase], mv_recv.at[phase, me], {"frac": target})
        send(lines, lines, mv_send.at[phase], pair_recv.at[phase], {"mat": sibling})
        sent.append((mv_ref.at[phase, :, 0, lines_sent], mv_send.at[phase]))
        sent.append((mv_ref.at[phase, pl.ds(0, n_frac - 1), 0, lines_sent], mv_send.at[phase]))

    def pass_on(phase):
        for source in near_first:
            lines = mv_ref.at[phase, source, core, lines_sent]
            take(lines, mv_recv.at[phase, source])
            send(lines, lines, mv_send.at[phase], pair_recv.at[phase], {"mat": sibling})

    def finish_matvec(phase, vector):
        take(mv_ref.at[phase, :, 0, lines_sent], pair_recv.at[phase])
        forward = mv_ref[phase, :, :, half * tiles_row : lines_half].reshape(blocks, size_b)
        product = total_of(vector * (diag * vector + forward))
        arrived = mv_ref[phase].reshape(n_frac * 2 * stride, size_b)
        both = sum(dot_nn(targets, part) for part in split_parts(arrived, 2))
        return product, diag * vector + 0.5 * both

    def set_row_hot():
        line = lax.broadcasted_iota(i32, (grid_rows, quarter), 0)
        for q in range(4):
            cut = slice(q * quarter, (q + 1) * quarter)
            row_hot_ref[:, cut] = as_hot(line == cell_row[:, cut])

    part_x = width_x // 4

    def set_sources(flux):
        wide = lane_hot_ref[...]
        weights = [wide * part for part in split_parts(flux, 2)]
        for q in range(4):
            low = q * part_x
            hot = row_hot_ref[low * width_y : (low + part_x) * width_y, :]
            total = sum(dot_nt(hot, weight) for weight in weights)
            base_ref[low : low + part_x] = msource_ref[low : low + part_x] + total.reshape(part_x, width_y, depth_z)

    begin = gathered(0)
    trace = traces()
    flux = kappa * (trace - at_slots(begin))
    scatter_share(0, [landed(flux)])

    tiles_copy.wait()
    start_matvec(0, begin)
    set_inverse()
    set_row_hot()
    msource_copy.wait()
    set_sources(flux)
    take(dest_in_ref.at[pl.ds(0, n_frac - 1)], vec_recv.at[3])
    block_line = lax.broadcasted_iota(i32, (blocks, LANES), 0)
    targets = jnp.concatenate(
        [as_hot(block_line == dest_in_ref[d].astype(i32))[:, : 2 * stride] for d in range(n_frac)], axis=1
    )
    fsource = gathered(1)
    diag = gathered(2)
    gather_share(0)
    pass_on(0)

    wait_halo(0)
    sweep_part(0, 0, width_x)
    send_halo(1)
    _, image = finish_matvec(0, begin)
    (loaded,) = whole_shares(0)
    residual = fsource + loaded - image
    fracture = begin

    def fill(number):
        if number == 0:
            wait_halo(1)
            sweep_part(1, 0, width_x)
            send_halo(2)
            set_parts(2)
            state["weight"] = landed(kappa)
        elif number == 1:
            state["trace"] = traces()
            scatter_share(1, [landed(kappa * state["trace"]), state["weight"]])
        elif number == 2:
            gather_share(1)
        elif number == 3:
            flux = kappa * (state["trace"] - at_slots(state["fracture"]))
            state["flux"] = flux
            set_sources(flux)
            wait_halo(2)
            sweep_part(2, 0, width_x)
            send_halo(3)
        elif number == 4:
            for g in range(groups):
                back_out_ref[g] = state["flux"][:, g * LANES : (g + 1) * LANES]
            spread_to_all(lambda target: back_out_ref.at[target // per], back_in_ref, back_send, back_recv)
            back_in_ref[me_dev] = back_out_ref[me_dev // per]
            wait_halo(3)
            sweep_part(3, 0, width_x)
        elif number == 5:
            take(back_in_ref.at[pl.ds(0, devices - 1)], back_recv)
            came = back_in_ref[...].reshape(devices, LANES)
            lines_back = sum(
                lax.dot_general(part, named_hot, (((0,), (0,)), ((), ())), preferred_element_type=f32)
                for part in split_parts(came, 3)
            )
            want = rank + capacity * lax.rem(me_dev, per)
            flux_out_ref[...] = jnp.sum(jnp.where(spot == want, lines_back, 0.0), axis=0, keepdims=True)

    state = {}
    last = OUTER * CG_ITERS - 1
    for number in range(OUTER * CG_ITERS):
        step = number % CG_ITERS
        phase = number + 1
        if number == CG_ITERS:
            traced, weight = whole_shares(1)
            residual = residual + ((traced - weight * fracture) - loaded)
            state["fracture"] = fracture
        if number < last:
            start_matvec(phase, residual)
        else:
            vector_ref[phase] = residual
            partial = jnp.zeros((1, size_b), f32)
            for r in range(rows):
                own = vector_ref[phase, pl.ds(me * rows + r, 1), :]
                partial = partial + own * tile_line(phase, r, None, None)
            part_out_ref[...] = partial
            spread_to_frac(part_out_ref, part_in_ref, part_send, part_recv)
            part_in_ref[me] = part_out_ref[...]
        norm_next = total_of(residual * residual)
        fill(number)
        if number < last:
            pass_on(phase)
            product, image = finish_matvec(phase, residual)
        else:
            take(part_in_ref.at[pl.ds(0, n_frac - 1)], part_recv)
            product = total_of(diag * residual * residual)
            lines_all = part_in_ref[0]
            for d in range(1, n_frac):
                lines_all = lines_all + part_in_ref[d]
            product = product + total_of(lines_all)
        if step == 0:
            alpha = norm_next / product
            direction = residual
            along = image
        else:
            ratio = norm_next / norm_now
            alpha = norm_next / (product - ratio * norm_next / alpha)
            direction = residual + ratio * direction
            if number < last:
                along = image + ratio * along
        norm_now = norm_next
        fracture = fracture + alpha * direction
        if number < last:
            residual = residual - alpha * along

    vector_ref[0] = fracture
    own_ref[...] = vector_ref[0, pl.ds(pl.multiple_of(me * rows, rows), rows), :]
    for ref, sem in sent:
        take(ref, sem)
    for copy in slow_sends:
        copy.wait_send()


def coupled(pressure, face, cell_coef, matrix_source, tiles, owner, cells, places, kappa, tile_cols, diag, begin, fsource):
    n_frac, n_mat = lax.axis_size("frac"), lax.axis_size("mat")
    devices = n_frac * n_mat
    rows, tiles_row, size_b = tiles.shape[0], tiles.shape[1], tiles.shape[3]
    blocks = rows * n_frac
    x, y, z = pressure.shape
    mortars = owner.shape[1]
    capacity = 2 * mortars // devices
    slots = devices * capacity
    groups = slots // LANES
    share = blocks // devices
    stride = -(-(rows // 2 * (tiles_row + 1)) // 8) * 8
    f32, bf16 = jnp.float32, jnp.bfloat16
    vmem = pl.BlockSpec(memory_space=pltpu.VMEM)
    smem = pl.BlockSpec(memory_space=pltpu.SMEM)
    hbm = pl.BlockSpec(memory_space=pltpu.HBM)
    phases = OUTER * CG_ITERS + 1
    sweeps = OUTER * SWEEPS
    dma = pltpu.SemaphoreType.DMA
    return pl.pallas_call(
        functools.partial(coupled_kernel, n_frac, n_mat),
        out_shape=(
            pltpu.VMEM((x, y, z), f32),
            pltpu.VMEM((rows, size_b), f32),
            pltpu.VMEM((1, mortars), f32),
        ),
        in_specs=[hbm] * 5 + [vmem] * 4 + [smem] + [vmem] * 3,
        out_specs=(vmem, vmem, vmem),
        scratch_shapes=[
            pltpu.VMEM((sweeps, x + 2, y, z), f32),
            pltpu.VMEM((x + 1, y, z), f32),
            pltpu.VMEM((x, y, z), f32),
            pltpu.VMEM((x, y, z), f32),
            pltpu.VMEM((x, y, z), f32),
            pltpu.VMEM((x, y, z), f32),
            pltpu.VMEM((x, y, z), f32),
            pltpu.VMEM((x, y, z), f32),
            pltpu.VMEM((rows, tiles_row, size_b, size_b), f32),
            pltpu.VMEM((2, x * y, z), bf16),
            pltpu.VMEM((x * y, slots), bf16),
            pltpu.VMEM((z, slots), bf16),
            pltpu.VMEM((sweeps, 2, x, z), f32),
            pltpu.VMEM((sweeps, 2, x, z), f32),
            pltpu.VMEM((x, z), f32),
            pltpu.VMEM((x, z), f32),
            pltpu.VMEM((devices, 1, LANES), f32),
            pltpu.VMEM((devices, 1, LANES), f32),
            pltpu.VMEM((3, n_frac, rows, size_b), f32),
            pltpu.VMEM((1, LANES), f32),
            pltpu.VMEM((n_frac, 1, LANES), f32),
            pltpu.VMEM((phases, n_frac, 2, stride, size_b), f32),
            pltpu.VMEM((phases, blocks, size_b), f32),
            pltpu.VMEM((devices, 1, share, size_b), f32),
            pltpu.VMEM((devices, 1, share, size_b), f32),
            pltpu.VMEM((devices, 1, share, size_b), f32),
            pltpu.VMEM((devices, 2, share, size_b), f32),
            pltpu.VMEM((devices, 2, share, size_b), f32),
            pltpu.VMEM((devices, 2, share, size_b), f32),
            pltpu.VMEM((1, size_b), f32),
            pltpu.VMEM((n_frac, 1, size_b), f32),
            pltpu.VMEM((groups, 1, LANES), f32),
            pltpu.VMEM((devices, 1, LANES), f32),
            dma((7,)),
            dma,
            dma,
            dma((4,)),
            dma((4,)),
            dma((phases,)),
            dma((phases, n_frac)),
            dma((phases,)),
            dma((2,)),
            dma((2,)),
            dma((2,)),
            dma((2,)),
            dma,
            dma,
            dma,
            dma,
            dma((sweeps + 1, 4)),
            dma((sweeps + 1, 4)),
        ],
        compiler_params=pltpu.CompilerParams(
            collective_id=0, has_side_effects=True, vmem_limit_bytes=60 * 1024 * 1024
        ),
        name="coupled",
    )(pressure, face, cell_coef, matrix_source, tiles, owner, cells, places, kappa, tile_cols, diag, begin, fsource)


def body(
    pressure_start,
    face_trans,
    cell_coef,
    matrix_source,
    mortar_owner,
    mortar_cell,
    mortar_frac,
    mortar_kappa,
    tiles,
    tile_cols,
    frac_diag,
    frac_source,
    fracture_start,
):
    size_b = tiles.shape[2]
    line = (1, -1)
    blocked = (-1, size_b)
    pressure, fracture, flux = coupled(
        pressure_start,
        face_trans,
        cell_coef,
        matrix_source,
        tiles,
        mortar_owner.reshape(line),
        mortar_cell.reshape(line),
        mortar_frac.reshape(line),
        mortar_kappa.reshape(line),
        tile_cols.T,
        frac_diag.reshape(blocked),
        fracture_start.reshape(blocked),
        frac_source.reshape(blocked),
    )
    return (pressure, fracture.reshape(-1), flux.reshape(-1))


def solution(mesh):
    in_specs = (
        P("mat", "frac", None),
        P(None, "mat", "frac", None),
        P("mat", "frac", None),
        P("mat", "frac", None),
        P(("mat", "frac"), None),
        P(("mat", "frac")),
        P(("mat", "frac")),
        P(("mat", "frac")),
        P("frac", None, None, None),
        P("frac", None),
        P("frac"),
        P("frac"),
        P("frac"),
    )
    out_specs = (P("mat", "frac", None), P("frac"), P(("mat", "frac")))
    return jax.shard_map(body, mesh=mesh, in_specs=in_specs, out_specs=out_specs, check_vma=False)
```

```python
import functools

import jax
import jax.numpy as jnp
from jax import lax
from jax.experimental import pallas as pl
from jax.experimental.pallas import tpu as pltpu
from jax.sharding import PartitionSpec as P

SWEEPS = 2
CG_ITERS = 3
OUTER = 2

MESH = pl.DeviceIdType.MESH
LANES = 128

relax_weight = 0.8


def split_parts(values, count):
    parts = []
    for _ in range(count - 1):
        part = values.astype(jnp.bfloat16)
        parts.append(part)
        values = values - part.astype(jnp.float32)
    parts.append(values.astype(jnp.bfloat16))
    return parts


def as_hot(mask):
    return mask.astype(jnp.float32).astype(jnp.bfloat16)


def dot_nn(a, b):
    return lax.dot_general(a, b, (((1,), (0,)), ((), ())), preferred_element_type=jnp.float32)


def dot_nt(a, b):
    return lax.dot_general(a, b, (((1,), (1,)), ((), ())), preferred_element_type=jnp.float32)


def total_of(values):
    return jnp.sum(values, axis=(0, 1), keepdims=True)


def coupled_kernel(n_frac, n_mat, *refs):
    (press_hbm, face_hbm, cell_hbm, msource_hbm, tiles_hbm, owner_hbm, cells_hbm, places_hbm, kappa_hbm, cols_hbm,
     diag_hbm, begin_hbm, fsource_hbm, out_ref, own_ref, flux_out_ref, *scratch) = refs
    (owner_ref, cells_ref, places_ref, kappa_in_ref, cols_ref, diag_ref, begin_ref, fsource_ref, targets_ref, grid_ref, tx_ref, ty_ref, tz_ref, inv_ref, cell_ref, msource_ref, base_ref, tiles_ref, parts_ref,
     row_hot_ref, lane_hot_ref, side_ref, edge_ref, ty_edge_ref, ty_side_ref, mort_out_ref, mort_in_ref, vec_ref,
     dest_out_ref, dest_in_ref, mv_ref, vector_ref, rs_out_0, rs_in_0, ag_0, rs_out_1, rs_in_1, ag_1, part_out_ref, part_in_ref,
     back_out_ref, back_in_ref, local_sem, mort_send, mort_recv, vec_send, vec_recv, mv_send, mv_recv,
     pair_recv, rs_send, rs_recv, ag_send, ag_recv, part_send, part_recv, back_send, back_recv, halo_send, halo_recv) = scratch
    rows, tiles_row, size_b = tiles_ref.shape[0], tiles_ref.shape[1], tiles_ref.shape[3]
    width_x, width_y, depth_z = inv_ref.shape
    grid_rows = width_x * width_y
    mortars = owner_ref.shape[1]
    devices = n_mat * n_frac
    capacity = 2 * mortars // devices
    per = LANES // capacity
    groups = devices // per
    slots = devices * capacity
    blocks = rows * n_frac
    half = rows // 2
    lines_half = half * tiles_row + half
    stride = -(-lines_half // 8) * 8
    share = blocks // devices
    sweeps = OUTER * SWEEPS
    f32, i32 = jnp.float32, jnp.int32
    me = lax.axis_index("frac")
    me_mat = lax.axis_index("mat")
    me_dev = me_mat * n_frac + me
    core = lax.rem(me_mat, 2)
    sibling = me_mat + 1 - 2 * core
    everyone = [(c, k) for c in range(n_mat) for k in range(n_frac) if c or k]

    barrier = pltpu.get_barrier_semaphore()
    for c, k in everyone:
        pl.semaphore_signal(
            barrier,
            inc=1,
            device_id={"mat": lax.rem(me_mat + c, n_mat), "frac": lax.rem(me + k, n_frac)},
            device_id_type=MESH,
        )

    def load(index, src, dst):
        copy = pltpu.make_async_copy(src, dst, local_sem.at[index])
        copy.start()
        return copy

    small_copies = [
        load(7, owner_hbm, owner_ref),
        load(8, cells_hbm, cells_ref),
        load(9, places_hbm, places_ref),
        load(10, kappa_hbm, kappa_in_ref),
        load(11, cols_hbm, cols_ref),
        load(12, begin_hbm, begin_ref),
        load(13, fsource_hbm, fsource_ref),
        load(14, diag_hbm, diag_ref),
    ]
    press_copy = load(0, press_hbm, grid_ref.at[0, pl.ds(1, width_x)])
    tx_copy = load(1, face_hbm.at[0], tx_ref.at[pl.ds(1, width_x)])
    ty_copy = load(2, face_hbm.at[1], ty_ref)
    tiles_copy = load(3, tiles_hbm, tiles_ref)
    tz_copy = load(4, face_hbm.at[2], tz_ref)
    cell_copy = load(5, cell_hbm, cell_ref)
    msource_copy = load(6, msource_hbm, msource_ref)

    sent = []

    def send(src, dst, send_sem, recv_sem, device):
        copy = pltpu.make_async_remote_copy(
            src_ref=src, dst_ref=dst, send_sem=send_sem, recv_sem=recv_sem, device_id=device, device_id_type=MESH
        )
        copy.start()
        return copy

    def take(ref, sem):
        pltpu.make_async_copy(ref, ref, sem).wait()

    def spread_to_all(source, landing, send_sem, recv_sem):
        for c, k in everyone:
            mat, frac = lax.rem(me_mat + c, n_mat), lax.rem(me + k, n_frac)
            send(source(mat * n_frac + frac), landing.at[me_dev], send_sem, recv_sem, {"mat": mat, "frac": frac})
        sent.append((landing.at[pl.ds(0, devices - 1)], send_sem))

    def spread_to_frac(source, landing, send_sem, recv_sem):
        for k in range(1, n_frac):
            send(source, landing.at[me], send_sem, recv_sem, {"frac": lax.rem(me + k, n_frac)})
        sent.append((landing.at[pl.ds(0, n_frac - 1)], send_sem))

    for copy in small_copies:
        copy.wait()
    owner = owner_ref[...]
    named = lax.broadcasted_iota(i32, (devices, mortars), 0) == owner
    named_hot = as_hot(named)
    before = as_hot(lax.broadcasted_iota(i32, (mortars, mortars), 0) <= lax.broadcasted_iota(i32, (mortars, mortars), 1))
    counts = dot_nn(named_hot, before)
    rank = jnp.sum(jnp.where(named, counts, 0.0), axis=0, keepdims=True).astype(i32) - 1
    spot = lax.broadcasted_iota(i32, (LANES, mortars), 0)
    word = lax.rem(spot // capacity + (per - lax.rem(me_dev, per)), per)
    payload = jnp.where(word == 0, cells_ref[...].astype(f32), jnp.where(word == 1, places_ref[...].astype(f32), kappa_in_ref[...]))
    payload = jnp.where((word < 3) & (lax.rem(spot, capacity) == rank), payload, 0.0)
    outgoing = sum(dot_nt(named_hot, part) for part in split_parts(payload, 3))
    mort_out_ref[...] = outgoing.reshape(devices, 1, LANES)

    lane_line = lax.broadcasted_iota(i32, (1, LANES), 1)
    target_row = jnp.full((1, LANES), -1, i32)
    for h in range(2):
        for n in range(lines_half):
            r, t = h * half + n // tiles_row, n % tiles_row
            block = cols_ref[t, r] if n < half * tiles_row else me * rows + h * half + n - half * tiles_row
            target_row = jnp.where(lane_line == h * stride + n, block, target_row)
    dest_out_ref[...] = target_row.astype(f32)

    if stride > lines_half:
        mv_ref[:, :, :, lines_half:, :] = jnp.zeros((mv_ref.shape[0], n_frac, 2, stride - lines_half, size_b), f32)

    pl.semaphore_wait(barrier, devices - 1)
    spread_to_all(lambda target: mort_out_ref.at[target], mort_in_ref, mort_send, mort_recv)
    mort_in_ref[me_dev] = mort_out_ref[me_dev]
    spread_to_frac(begin_ref, vec_ref.at[0], vec_send.at[0], vec_recv.at[0])
    spread_to_frac(dest_out_ref, dest_in_ref, vec_send.at[3], vec_recv.at[3])
    vec_ref[0, me] = begin_ref[...]
    dest_in_ref[me] = dest_out_ref[...]

    lanes = lax.broadcasted_iota(i32, (width_y, depth_z), 1)
    lines = lax.broadcasted_iota(i32, (width_y, depth_z), 0)
    next_mat, prev_mat = lax.rem(me_mat + 1, n_mat), lax.rem(me_mat + n_mat - 1, n_mat)
    next_frac, prev_frac = lax.rem(me + 1, n_frac), lax.rem(me + n_frac - 1, n_frac)
    halos = {}
    slow_sends = []

    def send_halo(sweep):
        sems = [(halo_send.at[sweep, d], halo_recv.at[sweep, d]) for d in range(4)]
        halos[sweep] = [
            send(grid_ref.at[sweep, width_x], grid_ref.at[sweep, 0], *sems[0], {"mat": next_mat}),
            send(grid_ref.at[sweep, 1], grid_ref.at[sweep, width_x + 1], *sems[1], {"mat": prev_mat}),
            send(edge_ref.at[sweep, 0], side_ref.at[sweep, 0], *sems[2], {"frac": next_frac}),
            send(edge_ref.at[sweep, 1], side_ref.at[sweep, 1], *sems[3], {"frac": prev_frac}),
        ]
        slow_sends.extend(halos[sweep])

    def wait_halo(sweep):
        for copy in halos[sweep]:
            copy.wait_recv()
        grid_ref[sweep, 0] = jnp.where(me_mat == 0, 0.0, grid_ref[sweep, 0])
        grid_ref[sweep, width_x + 1] = jnp.where(me_mat == n_mat - 1, 0.0, grid_ref[sweep, width_x + 1])
        side_ref[sweep, 0] = jnp.where(me == 0, 0.0, side_ref[sweep, 0])
        side_ref[sweep, 1] = jnp.where(me == n_frac - 1, 0.0, side_ref[sweep, 1])

    press_copy.wait()
    edge_ref[0, 0] = grid_ref[0, 1 : width_x + 1, width_y - 1, :]
    edge_ref[0, 1] = grid_ref[0, 1 : width_x + 1, 0, :]
    send_halo(0)
    tx_copy.wait()
    ty_copy.wait()
    ty_edge_ref[...] = ty_ref[:, width_y - 1, :]
    coef_copies = [
        send(tx_ref.at[width_x], tx_ref.at[0], halo_send.at[sweeps, 0], halo_recv.at[sweeps, 0], {"mat": next_mat}),
        send(ty_edge_ref, ty_side_ref, halo_send.at[sweeps, 2], halo_recv.at[sweeps, 2], {"frac": next_frac}),
    ]
    slow_sends.extend(coef_copies)
    spread_to_frac(fsource_ref, vec_ref.at[1], vec_send.at[1], vec_recv.at[1])
    spread_to_frac(diag_ref, vec_ref.at[2], vec_send.at[2], vec_recv.at[2])
    vec_ref[1, me] = fsource_ref[...]
    vec_ref[2, me] = diag_ref[...]

    def gathered(index):
        take(vec_ref.at[index, pl.ds(0, n_frac - 1)], vec_recv.at[index])
        return vec_ref[index].reshape(blocks, size_b)

    def set_parts(sweep):
        high, low = split_parts(grid_ref[sweep, 1 : width_x + 1].reshape(grid_rows, depth_z), 2)
        parts_ref[0] = high
        parts_ref[1] = low

    def set_inverse():
        tz_copy.wait()
        cell_copy.wait()
        for copy in coef_copies:
            copy.wait_recv()
        tx_ref[0] = jnp.where(me_mat == 0, 0.0, tx_ref[0])
        ty_side_ref[...] = jnp.where(me == 0, 0.0, ty_side_ref[...])

        def plane(x, carry):
            ty_here, tz_here = ty_ref[x], tz_ref[x]
            tz_in = jnp.where(lanes == depth_z - 1, 0.0, tz_here)
            ty_low = jnp.where(lines == 0, ty_side_ref[pl.ds(x, 1), :], pltpu.roll(ty_here, 1, 0))
            tz_low = pltpu.roll(tz_in, 1, 1)
            inv_ref[x] = relax_weight / (cell_ref[x] + tx_ref[x + 1] + tx_ref[x] + ty_here + ty_low + tz_here + tz_low)
            tz_ref[x] = tz_in
            return carry

        lax.fori_loop(0, width_x, plane, 0)

    def sweep_part(sweep, low, high):
        def plane(x, carry):
            here = grid_ref[sweep, x + 1]
            ty_here, tz_here = ty_ref[x], tz_ref[x]
            up = jnp.where(lines == width_y - 1, side_ref[sweep, 1, pl.ds(x, 1), :], pltpu.roll(here, width_y - 1, 0))
            down = jnp.where(
                lines == 0,
                ty_side_ref[pl.ds(x, 1), :] * side_ref[sweep, 0, pl.ds(x, 1), :],
                pltpu.roll(ty_here * here, 1, 0),
            )
            total = base_ref[x] + tx_ref[x + 1] * grid_ref[sweep, x + 2] + tx_ref[x] * grid_ref[sweep, x]
            total = total + ty_here * up + down
            total = total + tz_here * pltpu.roll(here, depth_z - 1, 1) + pltpu.roll(tz_here * here, 1, 1)
            value = (1.0 - relax_weight) * here + inv_ref[x] * total
            if sweep + 1 < sweeps:
                grid_ref[sweep + 1, x + 1] = value
                edge_ref[sweep + 1, 0, pl.ds(x, 1), :] = value[width_y - 1 :]
                edge_ref[sweep + 1, 1, pl.ds(x, 1), :] = value[:1]
            else:
                out_ref[x] = value
            return carry

        lax.fori_loop(low, high, plane, 0)

    set_parts(0)

    take(mort_in_ref.at[pl.ds(0, devices - 1)], mort_recv)
    arrived = mort_in_ref[...].reshape(devices, LANES)
    window = lax.broadcasted_iota(i32, (devices, LANES), 1) // capacity
    device = lax.broadcasted_iota(i32, (devices, LANES), 0)

    def slot_line(word_no):
        turned = pltpu.roll(arrived, LANES - word_no * capacity, 1) if word_no else arrived
        chosen = jnp.where(lax.rem(device, per) == window, turned, 0.0)
        return jnp.concatenate(
            [jnp.sum(chosen[g * per : (g + 1) * per], axis=0, keepdims=True) for g in range(groups)], axis=1
        )

    cell = slot_line(0).astype(i32)
    place = slot_line(1).astype(i32)
    kappa = slot_line(2)
    cell_row = cell // depth_z
    cell_lane = cell - cell_row * depth_z
    block_of = place // size_b
    lane_of = place - block_of * size_b
    lane_hot_ref[...] = as_hot(lax.broadcasted_iota(i32, (depth_z, slots), 0) == cell_lane)
    by_lane = as_hot(lax.broadcasted_iota(i32, (size_b, slots), 0) == lane_of)
    by_block = lax.broadcasted_iota(i32, (blocks, slots), 0) == block_of

    quarter = slots // 4
    grid_line = lax.broadcasted_iota(i32, (grid_rows, quarter), 0)

    def traces():
        found = []
        for q in range(4):
            hot = lane_hot_ref[:, q * quarter : (q + 1) * quarter]
            picked = dot_nn(parts_ref[0], hot) + dot_nn(parts_ref[1], hot)
            found.append(
                jnp.sum(jnp.where(grid_line == cell_row[:, q * quarter : (q + 1) * quarter], picked, 0.0), axis=0, keepdims=True)
            )
        return jnp.concatenate(found, axis=1)

    def at_slots(values):
        picked = sum(dot_nn(part, by_lane) for part in split_parts(values, 3))
        return jnp.sum(jnp.where(by_block, picked, 0.0), axis=0, keepdims=True)

    def landed(values):
        return sum(dot_nt(as_part, by_lane) for as_part in split_parts(jnp.where(by_block, values, 0.0), 3))

    shares = [(rs_out_0, rs_in_0, ag_0), (rs_out_1, rs_in_1, ag_1)]

    def scatter_share(stage, arrays):
        out, landing, _ = shares[stage]
        for n, array in enumerate(arrays):
            out[:, n] = array.reshape(devices, share, size_b)
        spread_to_all(lambda target: out.at[target], landing, rs_send.at[stage], rs_recv.at[stage])
        landing[me_dev] = out[me_dev]

    def gather_share(stage):
        _, landing, whole = shares[stage]
        take(landing.at[pl.ds(0, devices - 1)], rs_recv.at[stage])
        mine = landing[0]
        for d in range(1, devices):
            mine = mine + landing[d]
        whole[me_dev] = mine
        spread_to_all(lambda target: whole.at[me_dev], whole, ag_send.at[stage], ag_recv.at[stage])

    def whole_shares(stage):
        _, _, whole = shares[stage]
        take(whole.at[pl.ds(0, devices - 1)], ag_recv.at[stage])
        return [whole[:, n].reshape(blocks, size_b) for n in range(whole.shape[1])]

    def tile_line(phase, r, down, place):
        total = None
        for t in range(tiles_row):
            tile = tiles_ref[r, t]
            part = tile * vector_ref[phase, pl.ds(cols_ref[t, r], 1), :]
            total = part if total is None else total + part
            if place is not None:
                line = place * tiles_row + t
                mv_ref[phase, me, core, line : line + 1, :] = jnp.sum(tile * down, axis=0, keepdims=True)
        return jnp.sum(total.T, axis=0, keepdims=True)

    falling = [n_frac - 1 - n - (n_frac - 1 - n <= me).astype(i32) for n in range(n_frac - 1)]
    rising = [n + (n >= me).astype(i32) for n in range(n_frac - 1)]
    near_first = [jnp.where(2 * me < n_frac, up, down) for up, down in zip(rising, falling)]
    lines_sent = pl.ds(0, lines_half)

    def start_matvec(phase, vector):
        vector_ref[phase] = vector
        for n in range(half):
            r = core * half + n
            own = vector_ref[phase, pl.ds(me * rows + r, 1), :]
            forward = tile_line(phase, r, jnp.broadcast_to(own, (size_b, size_b)).T, n)
            line = half * tiles_row + n
            mv_ref[phase, me, core, line : line + 1, :] = forward
        lines = mv_ref.at[phase, me, core, lines_sent]
        for target in reversed(near_first):
            send(lines, lines, mv_send.at[phase], mv_recv.at[phase, me], {"frac": target})
        send(lines, lines, mv_send.at[phase], pair_recv.at[phase], {"mat": sibling})
        sent.append((mv_ref.at[phase, :, 0, lines_sent], mv_send.at[phase]))
        sent.append((mv_ref.at[phase, pl.ds(0, n_frac - 1), 0, lines_sent], mv_send.at[phase]))

    def pass_on(phase):
        for source in near_first:
            lines = mv_ref.at[phase, source, core, lines_sent]
            take(lines, mv_recv.at[phase, source])
            send(lines, lines, mv_send.at[phase], pair_recv.at[phase], {"mat": sibling})

    def combined(phase, side):
        arrived = mv_ref[phase, :, side].reshape(n_frac * stride, size_b)
        return sum(dot_nn(targets_ref[side], part) for part in split_parts(arrived, 2))

    def finish_matvec(phase, vector):
        direct = combined(phase, core)
        take(mv_ref.at[phase, :, 0, lines_sent], pair_recv.at[phase])
        forward = mv_ref[phase, :, :, half * tiles_row : lines_half].reshape(blocks, size_b)
        product = total_of(vector * (diag * vector + forward))
        return product, diag * vector + 0.5 * (direct + combined(phase, 1 - core))

    def set_row_hot():
        line = lax.broadcasted_iota(i32, (grid_rows, quarter), 0)
        for q in range(4):
            cut = slice(q * quarter, (q + 1) * quarter)
            row_hot_ref[:, cut] = as_hot(line == cell_row[:, cut])

    part_x = width_x // 4

    def set_sources(flux):
        wide = lane_hot_ref[...]
        weights = [wide * part for part in split_parts(flux, 2)]
        for q in range(4):
            low = q * part_x
            hot = row_hot_ref[low * width_y : (low + part_x) * width_y, :]
            total = sum(dot_nt(hot, weight) for weight in weights)
            base_ref[low : low + part_x] = msource_ref[low : low + part_x] + total.reshape(part_x, width_y, depth_z)

    begin = gathered(0)
    trace = traces()
    flux = kappa * (trace - at_slots(begin))
    scatter_share(0, [landed(flux)])

    tiles_copy.wait()
    start_matvec(0, begin)
    set_inverse()
    set_row_hot()
    msource_copy.wait()
    set_sources(flux)
    take(dest_in_ref.at[pl.ds(0, n_frac - 1)], vec_recv.at[3])
    block_line = lax.broadcasted_iota(i32, (blocks, LANES), 0)
    hots = [as_hot(block_line == dest_in_ref[d].astype(i32)) for d in range(n_frac)]
    for h in range(2):
        targets_ref[h] = jnp.concatenate([hot[:, h * stride : (h + 1) * stride] for hot in hots], axis=1)
    fsource = gathered(1)
    diag = gathered(2)
    gather_share(0)
    pass_on(0)

    wait_halo(0)
    sweep_part(0, 0, width_x)
    send_halo(1)
    _, image = finish_matvec(0, begin)
    (loaded,) = whole_shares(0)
    residual = fsource + loaded - image
    fracture = begin

    def fill(number):
        if number == 0:
            wait_halo(1)
            sweep_part(1, 0, width_x)
            send_halo(2)
            set_parts(2)
            state["weight"] = landed(kappa)
        elif number == 1:
            state["trace"] = traces()
            scatter_share(1, [landed(kappa * state["trace"]), state["weight"]])
        elif number == 2:
            gather_share(1)
        elif number == 3:
            flux = kappa * (state["trace"] - at_slots(state["fracture"]))
            state["flux"] = flux
            set_sources(flux)
            wait_halo(2)
            sweep_part(2, 0, width_x)
            send_halo(3)
        elif number == 4:
            for g in range(groups):
                back_out_ref[g] = state["flux"][:, g * LANES : (g + 1) * LANES]
            spread_to_all(lambda target: back_out_ref.at[target // per], back_in_ref, back_send, back_recv)
            back_in_ref[me_dev] = back_out_ref[me_dev // per]
            wait_halo(3)
            sweep_part(3, 0, width_x)
        elif number == 5:
            take(back_in_ref.at[pl.ds(0, devices - 1)], back_recv)
            came = back_in_ref[...].reshape(devices, LANES)
            lines_back = sum(
                lax.dot_general(part, named_hot, (((0,), (0,)), ((), ())), preferred_element_type=f32)
                for part in split_parts(came, 3)
            )
            want = rank + capacity * lax.rem(me_dev, per)
            flux_out_ref[...] = jnp.sum(jnp.where(spot == want, lines_back, 0.0), axis=0, keepdims=True)

    state = {}
    last = OUTER * CG_ITERS - 1
    for number in range(OUTER * CG_ITERS):
        step = number % CG_ITERS
        phase = number + 1
        if number == CG_ITERS:
            traced, weight = whole_shares(1)
            residual = residual + ((traced - weight * fracture) - loaded)
            state["fracture"] = fracture
        if number < last:
            start_matvec(phase, residual)
        else:
            vector_ref[phase] = residual
            partial = jnp.zeros((1, size_b), f32)
            for r in range(rows):
                own = vector_ref[phase, pl.ds(me * rows + r, 1), :]
                partial = partial + own * tile_line(phase, r, None, None)
            part_out_ref[...] = partial
            spread_to_frac(part_out_ref, part_in_ref, part_send, part_recv)
            part_in_ref[me] = part_out_ref[...]
        norm_next = total_of(residual * residual)
        fill(number)
        if number < last:
            pass_on(phase)
            product, image = finish_matvec(phase, residual)
        else:
            take(part_in_ref.at[pl.ds(0, n_frac - 1)], part_recv)
            product = total_of(diag * residual * residual)
            lines_all = part_in_ref[0]
            for d in range(1, n_frac):
                lines_all = lines_all + part_in_ref[d]
            product = product + total_of(lines_all)
        if step == 0:
            alpha = norm_next / product
            direction = residual
            along = image
        else:
            ratio = norm_next / norm_now
            alpha = norm_next / (product - ratio * norm_next / alpha)
            direction = residual + ratio * direction
            if number < last:
                along = image + ratio * along
        norm_now = norm_next
        fracture = fracture + alpha * direction
        if number < last:
            residual = residual - alpha * along

    vector_ref[0] = fracture
    own_ref[...] = vector_ref[0, pl.ds(pl.multiple_of(me * rows, rows), rows), :]
    for ref, sem in sent:
        take(ref, sem)
    for copy in slow_sends:
        copy.wait_send()


def coupled(pressure, face, cell_coef, matrix_source, tiles, owner, cells, places, kappa, tile_cols, diag, begin, fsource):
    n_frac, n_mat = lax.axis_size("frac"), lax.axis_size("mat")
    devices = n_frac * n_mat
    rows, tiles_row, size_b = tiles.shape[0], tiles.shape[1], tiles.shape[3]
    blocks = rows * n_frac
    x, y, z = pressure.shape
    mortars = owner.shape[1]
    capacity = 2 * mortars // devices
    slots = devices * capacity
    groups = slots // LANES
    share = blocks // devices
    stride = -(-(rows // 2 * (tiles_row + 1)) // 8) * 8
    f32, bf16 = jnp.float32, jnp.bfloat16
    vmem = pl.BlockSpec(memory_space=pltpu.VMEM)
    hbm = pl.BlockSpec(memory_space=pltpu.HBM)
    phases = OUTER * CG_ITERS + 1
    sweeps = OUTER * SWEEPS
    dma = pltpu.SemaphoreType.DMA
    return pl.pallas_call(
        functools.partial(coupled_kernel, n_frac, n_mat),
        out_shape=(
            pltpu.VMEM((x, y, z), f32),
            pltpu.VMEM((rows, size_b), f32),
            pltpu.VMEM((1, mortars), f32),
        ),
        in_specs=[hbm] * 13,
        out_specs=(vmem, vmem, vmem),
        scratch_shapes=[
            pltpu.VMEM((1, mortars), jnp.int32),
            pltpu.VMEM((1, mortars), jnp.int32),
            pltpu.VMEM((1, mortars), jnp.int32),
            pltpu.VMEM((1, mortars), f32),
            pltpu.SMEM((tiles_row, rows), jnp.int32),
            pltpu.VMEM((rows, size_b), f32),
            pltpu.VMEM((rows, size_b), f32),
            pltpu.VMEM((rows, size_b), f32),
            pltpu.VMEM((2, blocks, n_frac * stride), bf16),
            pltpu.VMEM((sweeps, x + 2, y, z), f32),
            pltpu.VMEM((x + 1, y, z), f32),
            pltpu.VMEM((x, y, z), f32),
            pltpu.VMEM((x, y, z), f32),
            pltpu.VMEM((x, y, z), f32),
            pltpu.VMEM((x, y, z), f32),
            pltpu.VMEM((x, y, z), f32),
            pltpu.VMEM((x, y, z), f32),
            pltpu.VMEM((rows, tiles_row, size_b, size_b), f32),
            pltpu.VMEM((2, x * y, z), bf16),
            pltpu.VMEM((x * y, slots), bf16),
            pltpu.VMEM((z, slots), bf16),
            pltpu.VMEM((sweeps, 2, x, z), f32),
            pltpu.VMEM((sweeps, 2, x, z), f32),
            pltpu.VMEM((x, z), f32),
            pltpu.VMEM((x, z), f32),
            pltpu.VMEM((devices, 1, LANES), f32),
            pltpu.VMEM((devices, 1, LANES), f32),
            pltpu.VMEM((3, n_frac, rows, size_b), f32),
            pltpu.VMEM((1, LANES), f32),
            pltpu.VMEM((n_frac, 1, LANES), f32),
            pltpu.VMEM((phases, n_frac, 2, stride, size_b), f32),
            pltpu.VMEM((phases, blocks, size_b), f32),
            pltpu.VMEM((devices, 1, share, size_b), f32),
            pltpu.VMEM((devices, 1, share, size_b), f32),
            pltpu.VMEM((devices, 1, share, size_b), f32),
            pltpu.VMEM((devices, 2, share, size_b), f32),
            pltpu.VMEM((devices, 2, share, size_b), f32),
            pltpu.VMEM((devices, 2, share, size_b), f32),
            pltpu.VMEM((1, size_b), f32),
            pltpu.VMEM((n_frac, 1, size_b), f32),
            pltpu.VMEM((groups, 1, LANES), f32),
            pltpu.VMEM((devices, 1, LANES), f32),
            dma((15,)),
            dma,
            dma,
            dma((4,)),
            dma((4,)),
            dma((phases,)),
            dma((phases, n_frac)),
            dma((phases,)),
            dma((2,)),
            dma((2,)),
            dma((2,)),
            dma((2,)),
            dma,
            dma,
            dma,
            dma,
            dma((sweeps + 1, 4)),
            dma((sweeps + 1, 4)),
        ],
        compiler_params=pltpu.CompilerParams(
            collective_id=0, has_side_effects=True, vmem_limit_bytes=60 * 1024 * 1024
        ),
        name="coupled",
    )(pressure, face, cell_coef, matrix_source, tiles, owner, cells, places, kappa, tile_cols, diag, begin, fsource)


def body(
    pressure_start,
    face_trans,
    cell_coef,
    matrix_source,
    mortar_owner,
    mortar_cell,
    mortar_frac,
    mortar_kappa,
    tiles,
    tile_cols,
    frac_diag,
    frac_source,
    fracture_start,
):
    size_b = tiles.shape[2]
    line = (1, -1)
    blocked = (-1, size_b)
    pressure, fracture, flux = coupled(
        pressure_start,
        face_trans,
        cell_coef,
        matrix_source,
        tiles,
        mortar_owner.reshape(line),
        mortar_cell.reshape(line),
        mortar_frac.reshape(line),
        mortar_kappa.reshape(line),
        tile_cols.T,
        frac_diag.reshape(blocked),
        fracture_start.reshape(blocked),
        frac_source.reshape(blocked),
    )
    return (pressure, fracture.reshape(-1), flux.reshape(-1))


def solution(mesh):
    in_specs = (
        P("mat", "frac", None),
        P(None, "mat", "frac", None),
        P("mat", "frac", None),
        P("mat", "frac", None),
        P(("mat", "frac"), None),
        P(("mat", "frac")),
        P(("mat", "frac")),
        P(("mat", "frac")),
        P("frac", None, None, None),
        P("frac", None),
        P("frac"),
        P("frac"),
        P("frac"),
    )
    out_specs = (P("mat", "frac", None), P("frac"), P(("mat", "frac")))
    return jax.shard_map(body, mesh=mesh, in_specs=in_specs, out_specs=out_specs, check_vma=False)
```

```python
import functools

import jax
import jax.numpy as jnp
from jax import lax
from jax.experimental import pallas as pl
from jax.experimental.pallas import tpu as pltpu
from jax.sharding import PartitionSpec as P

SWEEPS = 2
CG_ITERS = 3
OUTER = 2

MESH = pl.DeviceIdType.MESH
LANES = 128

relax_weight = 0.8


def split_parts(values, count):
    parts = []
    for _ in range(count - 1):
        part = values.astype(jnp.bfloat16)
        parts.append(part)
        values = values - part.astype(jnp.float32)
    parts.append(values.astype(jnp.bfloat16))
    return parts


def as_hot(mask):
    return mask.astype(jnp.float32).astype(jnp.bfloat16)


def dot_nn(a, b):
    return lax.dot_general(a, b, (((1,), (0,)), ((), ())), preferred_element_type=jnp.float32)


def dot_nt(a, b):
    return lax.dot_general(a, b, (((1,), (1,)), ((), ())), preferred_element_type=jnp.float32)


def total_of(values):
    return jnp.sum(values, axis=(0, 1), keepdims=True)


def coupled_kernel(n_frac, n_mat, *refs):
    (press_hbm, face_hbm, cell_hbm, msource_hbm, tiles_hbm, owner_hbm, cells_hbm, places_hbm, kappa_hbm, cols_hbm,
     diag_hbm, begin_hbm, fsource_hbm, out_ref, own_ref, flux_out_ref, *scratch) = refs
    (owner_ref, cells_ref, places_ref, kappa_in_ref, cols_ref, diag_ref, begin_ref, fsource_ref, targets_ref, grid_ref, tx_ref, ty_ref, tz_ref, inv_ref, cell_ref, msource_ref, base_ref, tiles_ref, parts_ref,
     row_hot_ref, lane_hot_ref, side_ref, edge_ref, ty_edge_ref, ty_side_ref, mort_out_ref, mort_in_ref, vec_ref,
     dest_out_ref, dest_in_ref, mv_ref, vector_ref, rs_out_0, rs_in_0, ag_0, rs_out_1, rs_in_1, ag_1, part_out_ref, part_in_ref,
     back_out_ref, back_in_ref, local_sem, mort_send, mort_recv, vec_send, vec_recv, mv_send, mv_recv,
     pair_recv, rs_send, rs_recv, ag_send, ag_recv, part_send, part_recv, back_send, back_recv, halo_send, halo_recv) = scratch
    rows, tiles_row, size_b = tiles_ref.shape[0], tiles_ref.shape[1], tiles_ref.shape[3]
    width_x, width_y, depth_z = inv_ref.shape
    grid_rows = width_x * width_y
    mortars = owner_ref.shape[1]
    devices = n_mat * n_frac
    capacity = 2 * mortars // devices
    per = LANES // capacity
    groups = devices // per
    slots = devices * capacity
    blocks = rows * n_frac
    half = rows // 2
    lines_half = half * tiles_row + half
    stride = -(-lines_half // 8) * 8
    share = blocks // devices
    sweeps = OUTER * SWEEPS
    f32, i32 = jnp.float32, jnp.int32
    me = lax.axis_index("frac")
    me_mat = lax.axis_index("mat")
    me_dev = me_mat * n_frac + me
    core = lax.rem(me_mat, 2)
    sibling = me_mat + 1 - 2 * core
    everyone = [(c, k) for c in range(n_mat) for k in range(n_frac) if c or k]

    barrier = pltpu.get_barrier_semaphore()
    for c, k in everyone:
        pl.semaphore_signal(
            barrier,
            inc=1,
            device_id={"mat": lax.rem(me_mat + c, n_mat), "frac": lax.rem(me + k, n_frac)},
            device_id_type=MESH,
        )

    def load(index, src, dst):
        copy = pltpu.make_async_copy(src, dst, local_sem.at[index])
        copy.start()
        return copy

    small_copies = [
        load(7, owner_hbm, owner_ref),
        load(8, cells_hbm, cells_ref),
        load(9, places_hbm, places_ref),
        load(10, kappa_hbm, kappa_in_ref),
        load(11, cols_hbm, cols_ref),
        load(12, begin_hbm, begin_ref),
        load(13, fsource_hbm, fsource_ref),
        load(14, diag_hbm, diag_ref),
    ]
    press_copy = load(0, press_hbm, grid_ref.at[0, pl.ds(1, width_x)])
    tx_copy = load(1, face_hbm.at[0], tx_ref.at[pl.ds(1, width_x)])
    ty_copy = load(2, face_hbm.at[1], ty_ref)
    tiles_copy = load(3, tiles_hbm, tiles_ref)
    tz_copy = load(4, face_hbm.at[2], tz_ref)
    cell_copy = load(5, cell_hbm, cell_ref)
    msource_copy = load(6, msource_hbm, msource_ref)

    sent = []

    def send(src, dst, send_sem, recv_sem, device):
        copy = pltpu.make_async_remote_copy(
            src_ref=src, dst_ref=dst, send_sem=send_sem, recv_sem=recv_sem, device_id=device, device_id_type=MESH
        )
        copy.start()
        return copy

    def take(ref, sem):
        pltpu.make_async_copy(ref, ref, sem).wait()

    def spread_to_all(source, landing, send_sem, recv_sem):
        for c, k in everyone:
            mat, frac = lax.rem(me_mat + c, n_mat), lax.rem(me + k, n_frac)
            arrival = recv_sem(frac) if callable(recv_sem) else recv_sem
            send(source(mat * n_frac + frac), landing.at[me_dev], send_sem, arrival, {"mat": mat, "frac": frac})
        sent.append((landing.at[pl.ds(0, devices - 1)], send_sem))

    def spread_to_frac(source, landing, send_sem, recv_sem):
        for k in range(1, n_frac):
            send(source, landing.at[me], send_sem, recv_sem, {"frac": lax.rem(me + k, n_frac)})
        sent.append((landing.at[pl.ds(0, n_frac - 1)], send_sem))

    sides = 2 if n_frac == 2 * per else 1
    my_side = me // per if sides == 2 else 0

    def side_from_here(frac):
        return lax.rem(frac // per + my_side, 2) if sides == 2 else 0

    def group_at(position):
        if sides == 1:
            return position
        return 2 * (position % n_mat) + lax.rem(my_side + position // n_mat, 2)

    def position_of(group):
        if sides == 1:
            return group
        return group // 2 + n_mat * lax.rem(lax.rem(group, 2) + my_side, 2)

    for copy in small_copies:
        copy.wait()
    owner = owner_ref[...]
    named = lax.broadcasted_iota(i32, (devices, mortars), 0) == owner
    named_hot = as_hot(named)
    before = as_hot(lax.broadcasted_iota(i32, (mortars, mortars), 0) <= lax.broadcasted_iota(i32, (mortars, mortars), 1))
    counts = dot_nn(named_hot, before)
    rank = jnp.sum(jnp.where(named, counts, 0.0), axis=0, keepdims=True).astype(i32) - 1
    spot = lax.broadcasted_iota(i32, (LANES, mortars), 0)
    word = lax.rem(spot // capacity + (per - lax.rem(me_dev, per)), per)
    payload = jnp.where(word == 0, cells_ref[...].astype(f32), jnp.where(word == 1, places_ref[...].astype(f32), kappa_in_ref[...]))
    payload = jnp.where((word < 3) & (lax.rem(spot, capacity) == rank), payload, 0.0)
    outgoing = sum(dot_nt(named_hot, part) for part in split_parts(payload, 3))
    mort_out_ref[...] = outgoing.reshape(devices, 1, LANES)

    lane_line = lax.broadcasted_iota(i32, (1, LANES), 1)
    target_row = jnp.full((1, LANES), -1, i32)
    for h in range(2):
        for n in range(lines_half):
            r, t = h * half + n // tiles_row, n % tiles_row
            block = cols_ref[t, r] if n < half * tiles_row else me * rows + h * half + n - half * tiles_row
            target_row = jnp.where(lane_line == h * stride + n, block, target_row)
    dest_out_ref[...] = target_row.astype(f32)

    if stride > lines_half:
        mv_ref[:, :, :, lines_half:, :] = jnp.zeros((mv_ref.shape[0], n_frac, 2, stride - lines_half, size_b), f32)

    pl.semaphore_wait(barrier, devices - 1)
    spread_to_all(lambda target: mort_out_ref.at[target], mort_in_ref, mort_send, lambda frac: mort_recv.at[side_from_here(frac)])
    mort_in_ref[me_dev] = mort_out_ref[me_dev]
    spread_to_frac(begin_ref, vec_ref.at[0], vec_send.at[0], vec_recv.at[0])
    spread_to_frac(dest_out_ref, dest_in_ref, vec_send.at[3], vec_recv.at[3])
    vec_ref[0, me] = begin_ref[...]
    dest_in_ref[me] = dest_out_ref[...]

    lanes = lax.broadcasted_iota(i32, (width_y, depth_z), 1)
    lines = lax.broadcasted_iota(i32, (width_y, depth_z), 0)
    next_mat, prev_mat = lax.rem(me_mat + 1, n_mat), lax.rem(me_mat + n_mat - 1, n_mat)
    next_frac, prev_frac = lax.rem(me + 1, n_frac), lax.rem(me + n_frac - 1, n_frac)
    halos = {}
    slow_sends = []

    def send_halo(sweep):
        sems = [(halo_send.at[sweep, d], halo_recv.at[sweep, d]) for d in range(4)]
        halos[sweep] = [
            send(grid_ref.at[sweep, width_x], grid_ref.at[sweep, 0], *sems[0], {"mat": next_mat}),
            send(grid_ref.at[sweep, 1], grid_ref.at[sweep, width_x + 1], *sems[1], {"mat": prev_mat}),
            send(edge_ref.at[sweep, 0], side_ref.at[sweep, 0], *sems[2], {"frac": next_frac}),
            send(edge_ref.at[sweep, 1], side_ref.at[sweep, 1], *sems[3], {"frac": prev_frac}),
        ]
        slow_sends.extend(halos[sweep])

    def wait_halo(sweep):
        for copy in halos[sweep]:
            copy.wait_recv()
        grid_ref[sweep, 0] = jnp.where(me_mat == 0, 0.0, grid_ref[sweep, 0])
        grid_ref[sweep, width_x + 1] = jnp.where(me_mat == n_mat - 1, 0.0, grid_ref[sweep, width_x + 1])
        side_ref[sweep, 0] = jnp.where(me == 0, 0.0, side_ref[sweep, 0])
        side_ref[sweep, 1] = jnp.where(me == n_frac - 1, 0.0, side_ref[sweep, 1])

    press_copy.wait()
    edge_ref[0, 0] = grid_ref[0, 1 : width_x + 1, width_y - 1, :]
    edge_ref[0, 1] = grid_ref[0, 1 : width_x + 1, 0, :]
    send_halo(0)
    tx_copy.wait()
    ty_copy.wait()
    ty_edge_ref[...] = ty_ref[:, width_y - 1, :]
    coef_copies = [
        send(tx_ref.at[width_x], tx_ref.at[0], halo_send.at[sweeps, 0], halo_recv.at[sweeps, 0], {"mat": next_mat}),
        send(ty_edge_ref, ty_side_ref, halo_send.at[sweeps, 2], halo_recv.at[sweeps, 2], {"frac": next_frac}),
    ]
    slow_sends.extend(coef_copies)
    spread_to_frac(fsource_ref, vec_ref.at[1], vec_send.at[1], vec_recv.at[1])
    spread_to_frac(diag_ref, vec_ref.at[2], vec_send.at[2], vec_recv.at[2])
    vec_ref[1, me] = fsource_ref[...]
    vec_ref[2, me] = diag_ref[...]

    def gathered(index):
        take(vec_ref.at[index, pl.ds(0, n_frac - 1)], vec_recv.at[index])
        return vec_ref[index].reshape(blocks, size_b)

    def set_parts(sweep):
        high, low = split_parts(grid_ref[sweep, 1 : width_x + 1].reshape(grid_rows, depth_z), 2)
        parts_ref[0] = high
        parts_ref[1] = low

    def set_inverse():
        tz_copy.wait()
        cell_copy.wait()
        for copy in coef_copies:
            copy.wait_recv()
        tx_ref[0] = jnp.where(me_mat == 0, 0.0, tx_ref[0])
        ty_side_ref[...] = jnp.where(me == 0, 0.0, ty_side_ref[...])

        def plane(x, carry):
            ty_here, tz_here = ty_ref[x], tz_ref[x]
            tz_in = jnp.where(lanes == depth_z - 1, 0.0, tz_here)
            ty_low = jnp.where(lines == 0, ty_side_ref[pl.ds(x, 1), :], pltpu.roll(ty_here, 1, 0))
            tz_low = pltpu.roll(tz_in, 1, 1)
            inv_ref[x] = relax_weight / (cell_ref[x] + tx_ref[x + 1] + tx_ref[x] + ty_here + ty_low + tz_here + tz_low)
            tz_ref[x] = tz_in
            return carry

        lax.fori_loop(0, width_x, plane, 0)

    def sweep_part(sweep, low, high):
        def plane(x, carry):
            here = grid_ref[sweep, x + 1]
            ty_here, tz_here = ty_ref[x], tz_ref[x]
            up = jnp.where(lines == width_y - 1, side_ref[sweep, 1, pl.ds(x, 1), :], pltpu.roll(here, width_y - 1, 0))
            down = jnp.where(
                lines == 0,
                ty_side_ref[pl.ds(x, 1), :] * side_ref[sweep, 0, pl.ds(x, 1), :],
                pltpu.roll(ty_here * here, 1, 0),
            )
            total = base_ref[x] + tx_ref[x + 1] * grid_ref[sweep, x + 2] + tx_ref[x] * grid_ref[sweep, x]
            total = total + ty_here * up + down
            total = total + tz_here * pltpu.roll(here, depth_z - 1, 1) + pltpu.roll(tz_here * here, 1, 1)
            value = (1.0 - relax_weight) * here + inv_ref[x] * total
            if sweep + 1 < sweeps:
                grid_ref[sweep + 1, x + 1] = value
                edge_ref[sweep + 1, 0, pl.ds(x, 1), :] = value[width_y - 1 :]
                edge_ref[sweep + 1, 1, pl.ds(x, 1), :] = value[:1]
            else:
                out_ref[x] = value
            return carry

        lax.fori_loop(low, high, plane, 0)

    set_parts(0)

    window = lax.broadcasted_iota(i32, (per, LANES), 1) // capacity
    device = lax.broadcasted_iota(i32, (per, LANES), 0)
    quarter = slots // 4
    grid_line = lax.broadcasted_iota(i32, (grid_rows, quarter), 0)

    def slot_lines(low, high):
        words = [[], [], []]
        for position in range(low, high):
            arrived = mort_in_ref[pl.ds(group_at(position) * per, per)].reshape(per, LANES)
            for n in range(3):
                turned = pltpu.roll(arrived, LANES - n * capacity, 1) if n else arrived
                words[n].append(jnp.sum(jnp.where(device == window, turned, 0.0), axis=0, keepdims=True))
        return [jnp.concatenate(word, axis=1) for word in words]

    def set_lane_hot(low, cells_here):
        row = cells_here // depth_z
        width = row.shape[1]
        lane_hot_ref[:, low : low + width] = as_hot(
            lax.broadcasted_iota(i32, (depth_z, width), 0) == cells_here - row * depth_z
        )
        return row

    def trace_quarter(q, rows_here):
        hot = lane_hot_ref[:, q * quarter : (q + 1) * quarter]
        picked = dot_nn(parts_ref[0], hot) + dot_nn(parts_ref[1], hot)
        return jnp.sum(jnp.where(grid_line == rows_here, picked, 0.0), axis=0, keepdims=True)

    found, row_list, place_list, kappa_list = [], [], [], []
    per_quarter = quarter // LANES
    for side in range(sides):
        count = devices // sides - (1 if side == 0 else 0)
        take(mort_in_ref.at[pl.ds(0, count)], mort_recv.at[side])
        first, last_group = side * groups // sides, (side + 1) * groups // sides
        cell_words, place_words, kappa_words = slot_lines(first, last_group)
        rows_here = set_lane_hot(first * LANES, cell_words.astype(i32))
        row_list.append(rows_here)
        place_list.append(place_words)
        kappa_list.append(kappa_words)
        for q in range(first // per_quarter, last_group // per_quarter):
            cut = q * quarter - first * LANES
            found.append(trace_quarter(q, rows_here[:, cut : cut + quarter]))
    cell_row = jnp.concatenate(row_list, axis=1)
    place = jnp.concatenate(place_list, axis=1).astype(i32)
    kappa = jnp.concatenate(kappa_list, axis=1)
    block_of = place // size_b
    lane_of = place - block_of * size_b
    by_lane = as_hot(lax.broadcasted_iota(i32, (size_b, slots), 0) == lane_of)
    by_block = lax.broadcasted_iota(i32, (blocks, slots), 0) == block_of

    def traces():
        return jnp.concatenate(
            [trace_quarter(q, cell_row[:, q * quarter : (q + 1) * quarter]) for q in range(4)], axis=1
        )

    def at_slots(values):
        picked = sum(dot_nn(part, by_lane) for part in split_parts(values, 3))
        return jnp.sum(jnp.where(by_block, picked, 0.0), axis=0, keepdims=True)

    def landed(values):
        return sum(dot_nt(as_part, by_lane) for as_part in split_parts(jnp.where(by_block, values, 0.0), 3))

    shares = [(rs_out_0, rs_in_0, ag_0), (rs_out_1, rs_in_1, ag_1)]

    def scatter_share(stage, arrays):
        out, landing, _ = shares[stage]
        for n, array in enumerate(arrays):
            out[:, n] = array.reshape(devices, share, size_b)
        spread_to_all(lambda target: out.at[target], landing, rs_send.at[stage], rs_recv.at[stage])
        landing[me_dev] = out[me_dev]

    def gather_share(stage):
        _, landing, whole = shares[stage]
        take(landing.at[pl.ds(0, devices - 1)], rs_recv.at[stage])
        mine = landing[0]
        for d in range(1, devices):
            mine = mine + landing[d]
        whole[me_dev] = mine
        spread_to_all(lambda target: whole.at[me_dev], whole, ag_send.at[stage], ag_recv.at[stage])

    def whole_shares(stage):
        _, _, whole = shares[stage]
        take(whole.at[pl.ds(0, devices - 1)], ag_recv.at[stage])
        return [whole[:, n].reshape(blocks, size_b) for n in range(whole.shape[1])]

    def tile_line(phase, r, down, place):
        total = None
        for t in range(tiles_row):
            tile = tiles_ref[r, t]
            part = tile * vector_ref[phase, pl.ds(cols_ref[t, r], 1), :]
            total = part if total is None else total + part
            if place is not None:
                line = place * tiles_row + t
                mv_ref[phase, me, core, line : line + 1, :] = jnp.sum(tile * down, axis=0, keepdims=True)
        return jnp.sum(total.T, axis=0, keepdims=True)

    falling = [n_frac - 1 - n - (n_frac - 1 - n <= me).astype(i32) for n in range(n_frac - 1)]
    rising = [n + (n >= me).astype(i32) for n in range(n_frac - 1)]
    near_first = [jnp.where(2 * me < n_frac, up, down) for up, down in zip(rising, falling)]
    lines_sent = pl.ds(0, lines_half)

    def start_matvec(phase, vector):
        vector_ref[phase] = vector
        for n in range(half):
            r = core * half + n
            own = vector_ref[phase, pl.ds(me * rows + r, 1), :]
            forward = tile_line(phase, r, jnp.broadcast_to(own, (size_b, size_b)).T, n)
            line = half * tiles_row + n
            mv_ref[phase, me, core, line : line + 1, :] = forward
        lines = mv_ref.at[phase, me, core, lines_sent]
        for target in reversed(near_first):
            send(lines, lines, mv_send.at[phase], mv_recv.at[phase, me], {"frac": target})
        send(lines, lines, mv_send.at[phase], pair_recv.at[phase], {"mat": sibling})
        sent.append((mv_ref.at[phase, :, 0, lines_sent], mv_send.at[phase]))
        sent.append((mv_ref.at[phase, pl.ds(0, n_frac - 1), 0, lines_sent], mv_send.at[phase]))

    def pass_on(phase):
        for source in near_first:
            lines = mv_ref.at[phase, source, core, lines_sent]
            take(lines, mv_recv.at[phase, source])
            send(lines, lines, mv_send.at[phase], pair_recv.at[phase], {"mat": sibling})

    def combined(phase, side):
        arrived = mv_ref[phase, :, side].reshape(n_frac * stride, size_b)
        return sum(dot_nn(targets_ref[side], part) for part in split_parts(arrived, 2))

    def finish_matvec(phase, vector):
        direct = combined(phase, core)
        take(mv_ref.at[phase, :, 0, lines_sent], pair_recv.at[phase])
        forward = mv_ref[phase, :, :, half * tiles_row : lines_half].reshape(blocks, size_b)
        product = total_of(vector * (diag * vector + forward))
        return product, diag * vector + 0.5 * (direct + combined(phase, 1 - core))

    def set_row_hot():
        line = lax.broadcasted_iota(i32, (grid_rows, quarter), 0)
        for q in range(4):
            cut = slice(q * quarter, (q + 1) * quarter)
            row_hot_ref[:, cut] = as_hot(line == cell_row[:, cut])

    part_x = width_x // 4

    def set_sources(flux):
        wide = lane_hot_ref[...]
        weights = [wide * part for part in split_parts(flux, 2)]
        for q in range(4):
            low = q * part_x
            hot = row_hot_ref[low * width_y : (low + part_x) * width_y, :]
            total = sum(dot_nt(hot, weight) for weight in weights)
            base_ref[low : low + part_x] = msource_ref[low : low + part_x] + total.reshape(part_x, width_y, depth_z)

    begin = gathered(0)
    trace = jnp.concatenate(found, axis=1)
    flux = kappa * (trace - at_slots(begin))
    scatter_share(0, [landed(flux)])

    tiles_copy.wait()
    start_matvec(0, begin)
    set_inverse()
    set_row_hot()
    msource_copy.wait()
    set_sources(flux)
    take(dest_in_ref.at[pl.ds(0, n_frac - 1)], vec_recv.at[3])
    block_line = lax.broadcasted_iota(i32, (blocks, LANES), 0)
    hots = [as_hot(block_line == dest_in_ref[d].astype(i32)) for d in range(n_frac)]
    for h in range(2):
        targets_ref[h] = jnp.concatenate([hot[:, h * stride : (h + 1) * stride] for hot in hots], axis=1)
    fsource = gathered(1)
    diag = gathered(2)
    gather_share(0)
    pass_on(0)

    wait_halo(0)
    sweep_part(0, 0, width_x)
    send_halo(1)
    _, image = finish_matvec(0, begin)
    (loaded,) = whole_shares(0)
    residual = fsource + loaded - image
    fracture = begin

    def fill(number):
        if number == 0:
            wait_halo(1)
            sweep_part(1, 0, width_x)
            send_halo(2)
            set_parts(2)
            state["weight"] = landed(kappa)
        elif number == 1:
            state["trace"] = traces()
            scatter_share(1, [landed(kappa * state["trace"]), state["weight"]])
        elif number == 2:
            gather_share(1)
        elif number == 3:
            flux = kappa * (state["trace"] - at_slots(state["fracture"]))
            state["flux"] = flux
            set_sources(flux)
            wait_halo(2)
            sweep_part(2, 0, width_x)
            send_halo(3)
        elif number == 4:
            for g in range(groups):
                back_out_ref[g] = state["flux"][:, g * LANES : (g + 1) * LANES]
            spread_to_all(lambda target: back_out_ref.at[position_of(target // per)], back_in_ref, back_send, back_recv)
            back_in_ref[me_dev] = back_out_ref[position_of(me_dev // per)]
            wait_halo(3)
            sweep_part(3, 0, width_x)
        elif number == 5:
            take(back_in_ref.at[pl.ds(0, devices - 1)], back_recv)
            came = back_in_ref[...].reshape(devices, LANES)
            lines_back = sum(
                lax.dot_general(part, named_hot, (((0,), (0,)), ((), ())), preferred_element_type=f32)
                for part in split_parts(came, 3)
            )
            want = rank + capacity * lax.rem(me_dev, per)
            flux_out_ref[...] = jnp.sum(jnp.where(spot == want, lines_back, 0.0), axis=0, keepdims=True)

    state = {}
    last = OUTER * CG_ITERS - 1
    for number in range(OUTER * CG_ITERS):
        step = number % CG_ITERS
        phase = number + 1
        if number == CG_ITERS:
            traced, weight = whole_shares(1)
            residual = residual + ((traced - weight * fracture) - loaded)
            state["fracture"] = fracture
        if number < last:
            start_matvec(phase, residual)
        else:
            vector_ref[phase] = residual
            partial = jnp.zeros((1, size_b), f32)
            for r in range(rows):
                own = vector_ref[phase, pl.ds(me * rows + r, 1), :]
                partial = partial + own * tile_line(phase, r, None, None)
            part_out_ref[...] = partial
            spread_to_frac(part_out_ref, part_in_ref, part_send, part_recv)
            part_in_ref[me] = part_out_ref[...]
        norm_next = total_of(residual * residual)
        fill(number)
        if number < last:
            pass_on(phase)
            product, image = finish_matvec(phase, residual)
        else:
            take(part_in_ref.at[pl.ds(0, n_frac - 1)], part_recv)
            product = total_of(diag * residual * residual)
            lines_all = part_in_ref[0]
            for d in range(1, n_frac):
                lines_all = lines_all + part_in_ref[d]
            product = product + total_of(lines_all)
        if step == 0:
            alpha = norm_next / product
            direction = residual
            along = image
        else:
            ratio = norm_next / norm_now
            alpha = norm_next / (product - ratio * norm_next / alpha)
            direction = residual + ratio * direction
            if number < last:
                along = image + ratio * along
        norm_now = norm_next
        fracture = fracture + alpha * direction
        if number < last:
            residual = residual - alpha * along

    vector_ref[0] = fracture
    own_ref[...] = vector_ref[0, pl.ds(pl.multiple_of(me * rows, rows), rows), :]
    for ref, sem in sent:
        take(ref, sem)
    for copy in slow_sends:
        copy.wait_send()


def coupled(pressure, face, cell_coef, matrix_source, tiles, owner, cells, places, kappa, tile_cols, diag, begin, fsource):
    n_frac, n_mat = lax.axis_size("frac"), lax.axis_size("mat")
    devices = n_frac * n_mat
    rows, tiles_row, size_b = tiles.shape[0], tiles.shape[1], tiles.shape[3]
    blocks = rows * n_frac
    x, y, z = pressure.shape
    mortars = owner.shape[1]
    capacity = 2 * mortars // devices
    slots = devices * capacity
    groups = slots // LANES
    share = blocks // devices
    stride = -(-(rows // 2 * (tiles_row + 1)) // 8) * 8
    f32, bf16 = jnp.float32, jnp.bfloat16
    vmem = pl.BlockSpec(memory_space=pltpu.VMEM)
    hbm = pl.BlockSpec(memory_space=pltpu.HBM)
    phases = OUTER * CG_ITERS + 1
    sweeps = OUTER * SWEEPS
    dma = pltpu.SemaphoreType.DMA
    return pl.pallas_call(
        functools.partial(coupled_kernel, n_frac, n_mat),
        out_shape=(
            pltpu.VMEM((x, y, z), f32),
            pltpu.VMEM((rows, size_b), f32),
            pltpu.VMEM((1, mortars), f32),
        ),
        in_specs=[hbm] * 13,
        out_specs=(vmem, vmem, vmem),
        scratch_shapes=[
            pltpu.VMEM((1, mortars), jnp.int32),
            pltpu.VMEM((1, mortars), jnp.int32),
            pltpu.VMEM((1, mortars), jnp.int32),
            pltpu.VMEM((1, mortars), f32),
            pltpu.SMEM((tiles_row, rows), jnp.int32),
            pltpu.VMEM((rows, size_b), f32),
            pltpu.VMEM((rows, size_b), f32),
            pltpu.VMEM((rows, size_b), f32),
            pltpu.VMEM((2, blocks, n_frac * stride), bf16),
            pltpu.VMEM((sweeps, x + 2, y, z), f32),
            pltpu.VMEM((x + 1, y, z), f32),
            pltpu.VMEM((x, y, z), f32),
            pltpu.VMEM((x, y, z), f32),
            pltpu.VMEM((x, y, z), f32),
            pltpu.VMEM((x, y, z), f32),
            pltpu.VMEM((x, y, z), f32),
            pltpu.VMEM((x, y, z), f32),
            pltpu.VMEM((rows, tiles_row, size_b, size_b), f32),
            pltpu.VMEM((2, x * y, z), bf16),
            pltpu.VMEM((x * y, slots), bf16),
            pltpu.VMEM((z, slots), bf16),
            pltpu.VMEM((sweeps, 2, x, z), f32),
            pltpu.VMEM((sweeps, 2, x, z), f32),
            pltpu.VMEM((x, z), f32),
            pltpu.VMEM((x, z), f32),
            pltpu.VMEM((devices, 1, LANES), f32),
            pltpu.VMEM((devices, 1, LANES), f32),
            pltpu.VMEM((3, n_frac, rows, size_b), f32),
            pltpu.VMEM((1, LANES), f32),
            pltpu.VMEM((n_frac, 1, LANES), f32),
            pltpu.VMEM((phases, n_frac, 2, stride, size_b), f32),
            pltpu.VMEM((phases, blocks, size_b), f32),
            pltpu.VMEM((devices, 1, share, size_b), f32),
            pltpu.VMEM((devices, 1, share, size_b), f32),
            pltpu.VMEM((devices, 1, share, size_b), f32),
            pltpu.VMEM((devices, 2, share, size_b), f32),
            pltpu.VMEM((devices, 2, share, size_b), f32),
            pltpu.VMEM((devices, 2, share, size_b), f32),
            pltpu.VMEM((1, size_b), f32),
            pltpu.VMEM((n_frac, 1, size_b), f32),
            pltpu.VMEM((groups, 1, LANES), f32),
            pltpu.VMEM((devices, 1, LANES), f32),
            dma((15,)),
            dma,
            dma((2,)),
            dma((4,)),
            dma((4,)),
            dma((phases,)),
            dma((phases, n_frac)),
            dma((phases,)),
            dma((2,)),
            dma((2,)),
            dma((2,)),
            dma((2,)),
            dma,
            dma,
            dma,
            dma,
            dma((sweeps + 1, 4)),
            dma((sweeps + 1, 4)),
        ],
        compiler_params=pltpu.CompilerParams(
            collective_id=0, has_side_effects=True, vmem_limit_bytes=60 * 1024 * 1024
        ),
        name="coupled",
    )(pressure, face, cell_coef, matrix_source, tiles, owner, cells, places, kappa, tile_cols, diag, begin, fsource)


def body(
    pressure_start,
    face_trans,
    cell_coef,
    matrix_source,
    mortar_owner,
    mortar_cell,
    mortar_frac,
    mortar_kappa,
    tiles,
    tile_cols,
    frac_diag,
    frac_source,
    fracture_start,
):
    size_b = tiles.shape[2]
    line = (1, -1)
    blocked = (-1, size_b)
    pressure, fracture, flux = coupled(
        pressure_start,
        face_trans,
        cell_coef,
        matrix_source,
        tiles,
        mortar_owner.reshape(line),
        mortar_cell.reshape(line),
        mortar_frac.reshape(line),
        mortar_kappa.reshape(line),
        tile_cols.T,
        frac_diag.reshape(blocked),
        fracture_start.reshape(blocked),
        frac_source.reshape(blocked),
    )
    return (pressure, fracture.reshape(-1), flux.reshape(-1))


def solution(mesh):
    in_specs = (
        P("mat", "frac", None),
        P(None, "mat", "frac", None),
        P("mat", "frac", None),
        P("mat", "frac", None),
        P(("mat", "frac"), None),
        P(("mat", "frac")),
        P(("mat", "frac")),
        P(("mat", "frac")),
        P("frac", None, None, None),
        P("frac", None),
        P("frac"),
        P("frac"),
        P("frac"),
    )
    out_specs = (P("mat", "frac", None), P("frac"), P(("mat", "frac")))
    return jax.shard_map(body, mesh=mesh, in_specs=in_specs, out_specs=out_specs, check_vma=False)
```
